128 devices in a mesh: row: 8 (over x_hi, y), col: 16 (over z, x_lo, core).
Axes of the slice: x: 4 (x_hi: 2, x_lo: 2; x = x_hi * 2 + x_lo), y: 4, z: 4, core: 2. Of those that a mesh axis runs over, the one named last changes fastest.
Arguments:
- velocity: float32 [3, 16, 16, 36, 32, 512], P(None, 'col', 'row'), may hold values from -6 to 6
- y_sizes: int32 [16], replicated, may hold values from 1 to 36, 512 in all
- old_place: int32 [16, 16], replicated, may hold values from 0 to 15, each once within a row
- new_col: int32 [16, 16], replicated, may hold values from 0 to 15, each once within a row
Outputs:
- divergence: float32 [16, 16, 2, 512, 512], P('row', 'col')
- peak: float32 [512, 512], replicated
The draws below stay inside these ranges and needn't reach their ends.
Inputs may be any that keep to these rules, and one draw needn't show every extreme that they name: `y_sizes`: the heights sum to 512 and the tallest is exactly 36. `old_place`: each row is a permutation of 0 to 15. `new_col`: each row is a permutation of 0 to 16 - 1.
All inputs are finite; a program needn't handle non-finite values.
Results may differ from the reference program's by a relative error of at most 0.0003.
Values sent between devices are 32-bit elements; how exact they have to be, the bound alone decides.
No kernel may reach another device: no remote copies, remote signals or barrier semaphores. Data moves between devices by JAX's collectives and lax.ppermute only.
A program may use at most 320 MiB of HBM per device.

```python
import math
import jax
import jax.numpy as jnp
import numpy as np
from jax import lax

NX = 512
ZB = 32
YCAP = 36
NBZ = 16
NBY = 16
NY = 512
N_COL = 16


def block_levels(own_key, dims, pieces, low, top_value):
    def one(axis_at, blocks):
        heights = jax.random.uniform(jax.random.fold_in(jax.random.fold_in(own_key, 6), axis_at), (blocks,), jnp.float32, low / len(pieces), top_value / len(pieces))
        return jnp.repeat(jnp.exp(heights), dims[axis_at] // blocks).reshape((-1,) + (1,) * (len(dims) - axis_at - 1))

    gain = one(*pieces[0])
    for cut in pieces[1:]:
        gain = gain * one(*cut)
    return gain


def split_up(amount, total, limit, slope):
    portions = [(1 << 20) // math.isqrt(grade ** slope) + 1 for grade in range(2, amount + 1)]
    rest, given = total - limit - (amount - 1), [1] * (amount - 1)
    while rest > 0:
        candidates = [i for i in range(amount - 1) if given[i] < limit]
        mass, budget = sum([portions[i] for i in candidates]), rest
        for i in candidates:
            more = min(limit - given[i], max(1, budget * portions[i] // mass), rest)
            given[i] = given[i] + more
            rest = rest - more
    return np.array([limit] + given)


def ragged_sizes(key, amount, total, most, slope):
    if amount == 2:
        one = jax.random.randint(key, (), max(1, total - most), min(most, total - 1) + 1)
        return jnp.stack([one, total - one])
    sizes = jnp.asarray(split_up(amount, total, most, slope), jnp.int32)
    twos = (amount - 1) // 2
    donor, receiver = sizes[1:1 + 2 * twos:2], sizes[2:2 + 2 * twos:2]
    slack = jnp.minimum(donor - 1, most - receiver)
    moved = jax.random.randint(jax.random.fold_in(key, 1), (twos,), 0, 1 << 20) % (slack + 1)
    sizes = sizes.at[1:1 + 2 * twos:2].set(donor - moved).at[2:2 + 2 * twos:2].set(receiver + moved)
    return sizes[jax.random.permutation(jax.random.fold_in(key, 2), amount)]


def normal_values(stream_key, extent, scale, most, cuts=(), kind=jnp.bfloat16):
    loudness = block_levels(stream_key, extent, cuts, -0.22, 0.18) if cuts else 1.0
    drawn = jax.random.normal(stream_key, extent, jnp.float32) * scale * loudness
    return jnp.minimum(jnp.maximum(drawn, -most), most).astype(kind)


def setup_inputs(seed: int = 0) -> dict:
    key_of = jax.random.split(jax.random.key(seed), 5)
    velocity = normal_values(key_of[0], (3, NBZ, NBY, YCAP, ZB, NX), 1.0, 6.0, ((1, 16), (2, 8)), jnp.float32)
    y_sizes = ragged_sizes(key_of[1], NBY, NY, YCAP, 1).astype(jnp.int32)
    old_place = jax.vmap(lambda own: jax.random.permutation(own, NBY))(jax.random.split(key_of[2], NBZ)).reshape((NBZ, NBY)).astype(jnp.int32)
    new_col = jax.vmap(lambda own: jax.random.permutation(own, N_COL))(jax.random.split(key_of[3], NBZ)).reshape((NBZ, N_COL)).astype(jnp.int32)
    return {"velocity": velocity, "y_sizes": y_sizes, "old_place": old_place, "new_col": new_col}


def derive(field, axis):
    count = field.shape[axis]
    spectrum = jnp.fft.rfft(field, axis=axis)
    modes = jnp.arange(count // 2 + 1)
    wave = jnp.where(modes == count // 2, 0, modes).astype(field.dtype) * (4.0 / count)
    shape = [1] * field.ndim
    shape[axis] = count // 2 + 1
    spectrum = spectrum * (1j * wave.reshape(shape))
    return jnp.fft.irfft(spectrum, n=count, axis=axis).astype(field.dtype)


def source_rows(y_sizes, old_place, row_depth, height):
    ends = jnp.cumsum(y_sizes).astype(jnp.int32)
    starts = (ends - y_sizes).astype(jnp.int32)
    cells = jnp.arange(height, dtype=jnp.int32)
    block = jnp.sum((cells[:, None] >= ends[None, :]).astype(jnp.int32), axis=1).astype(jnp.int32)
    offset = cells - jnp.take(starts, block)
    return (jnp.take(old_place, block, axis=1) * row_depth + offset).astype(jnp.int32)


def assemble(pair):
    block, index = pair
    flat = block.reshape(-1, block.shape[2], block.shape[3])
    return jnp.transpose(jnp.take(flat, index, axis=0), (1, 0, 2))


def reference(velocity, y_sizes, old_place, new_col):
    row_depth = velocity.shape[3]
    rows = source_rows(y_sizes, old_place, row_depth, NY)
    vertical = lax.map(assemble, (velocity[2], rows)).reshape(-1, NY, NX)
    slope_z = derive(vertical, 0).reshape(N_COL, ZB, NY, NX)

    def combine(group):
        block_x, block_y, index, part_z = group
        slope_x = derive(assemble((block_x, index)), 2)
        slope_y = derive(assemble((block_y, index)), 1)
        return slope_x + slope_y + part_z

    field = lax.map(combine, (velocity[0], velocity[1], rows, slope_z))
    peak = jnp.max(jnp.abs(field), axis=(0, 1))
    field = field.reshape(N_COL, N_COL, ZB // N_COL, NY, NX)
    hits = (new_col[:, :, None] == jnp.arange(N_COL, dtype=jnp.int32)[None, None, :]).astype(jnp.int32)
    slab_of = jnp.sum(hits * jnp.arange(N_COL, dtype=jnp.int32)[None, :, None], axis=1).astype(jnp.int32)
    divergence = jnp.take_along_axis(field, slab_of[:, :, None, None, None], axis=1)
    return (divergence, peak)
```

```python
import jax
import jax.numpy as jnp
import numpy as np
from jax import lax
from jax.experimental import pallas as pl
from jax.experimental.pallas import tpu as pltpu
from jax.sharding import PartitionSpec as P

AXES = ("row", "col")
LANES = 128
N = 512
DEVICES = 128
KX = N // DEVICES
ROWS = 72
CAP = 36
ZB = 32
NB = 16
NR = 8


def spectral_pair():
    gap = (np.arange(N)[:, None] - np.arange(N)[None, :]) % N
    angle = gap * (np.pi / N)
    parity = 1.0 - 2.0 * (gap % 2)
    safe = np.where(gap == 0, 1.0, np.sin(angle))
    full = np.where(gap == 0, 0.0, parity * np.cos(angle) / safe * (2.0 / N))
    full = (full - full.T) / 2
    high = full.astype(jnp.bfloat16)
    low = (full - high.astype(np.float64)).astype(jnp.bfloat16)
    return high, low


def halves(value):
    high = value.astype(jnp.bfloat16)
    return high, (value - high.astype(jnp.float32)).astype(jnp.bfloat16)


def mul(left, right):
    return jnp.dot(left, right, preferred_element_type=jnp.float32)


def mul3(left, right):
    return mul(left[0], right[0]) + (mul(left[1], right[0]) + mul(left[0], right[1]))


def pack_rows(value, out_ref, i):
    tall = jnp.concatenate([value[:, k * LANES : (k + 1) * LANES] for k in range(KX)], axis=0)
    out_ref[:, i, :] = tall.T


def pack_plain(in_ref, out_ref):
    for i in range(8):
        pack_rows(in_ref[0, i], out_ref, i)


def pack_slope(in_ref, high_ref, low_ref, out_ref):
    flat = in_ref[0].reshape(8 * ZB, N)
    slope = -mul3(halves(flat), (high_ref[...], low_ref[...]))
    for i in range(8):
        pack_rows(slope[i * ZB : (i + 1) * ZB], out_ref, i)


def pack(velocity, field, matrices=None):
    specs = [pl.BlockSpec((1, 8, ZB, N), lambda t: (field, t, 0, 0))]
    args = [velocity]
    if matrices is not None:
        specs += [pl.BlockSpec((N, N), lambda t: (0, 0))] * 2
        args += list(matrices)
    return pl.pallas_call(
        pack_plain if matrices is None else pack_slope,
        grid=(ROWS // 8,),
        in_specs=specs,
        out_specs=pl.BlockSpec((DEVICES, 8, LANES), lambda t: (0, t, 0)),
        out_shape=jax.ShapeDtypeStruct((DEVICES, ROWS, LANES), jnp.float32),
        name="pack_slope" if matrices is not None else f"pack_{field}",
        cost_estimate=pl.CostEstimate(
            flops=2 * ROWS * ZB * N * N * (6 if matrices is not None else 1),
            bytes_accessed=2 * ROWS * ZB * N * 4,
            transcendentals=0,
        ),
    )(*args)


def gather_quad(starts, places, in_ref, lined, quad):
    for cc in range(4):
        for b in range(NB):
            place = places[quad * 4 + cc, b]
            source = in_ref[place // 2, cc, pl.ds((place % 2) * CAP, CAP), :]
            lined[cc, pl.ds(starts[b], CAP), :] = source


def turn_lanes(parts):
    lane = lax.broadcasted_iota(jnp.int32, parts[0].shape, 1)
    upper = (lane // 64) == 1
    odd = (lane // 32) % 2 == 1
    a0, a1, a2, a3 = parts
    b0 = jnp.where(upper, pltpu.roll(a2, 64, 1), a0)
    b2 = jnp.where(upper, a2, pltpu.roll(a0, 64, 1))
    b1 = jnp.where(upper, pltpu.roll(a3, 64, 1), a1)
    b3 = jnp.where(upper, a3, pltpu.roll(a1, 64, 1))
    c0 = jnp.where(odd, pltpu.roll(b1, 32, 1), b0)
    c1 = jnp.where(odd, b1, pltpu.roll(b0, 96, 1))
    c2 = jnp.where(odd, pltpu.roll(b3, 32, 1), b2)
    c3 = jnp.where(odd, b3, pltpu.roll(b2, 96, 1))
    return c0, c1, c2, c3


CHUNK = 64


def gather_kernel(starts, places, in_ref, out_ref, lined):
    gather_quad(starts, places, in_ref, lined, pl.program_id(0))

    def step(t, carry):
        rows = pl.ds(pl.multiple_of(t * CHUNK, CHUNK), CHUNK)
        turned = turn_lanes([lined[cc, rows, :] for cc in range(4)])
        for k in range(KX):
            out_ref[k, rows, :] = turned[k]
        return carry

    lax.fori_loop(0, N // CHUNK, step, 0)


LINED = 560


def gather(received, starts, places, name):
    return pl.pallas_call(
        gather_kernel,
        grid_spec=pltpu.PrefetchScalarGridSpec(
            num_scalar_prefetch=2,
            grid=(4,),
            in_specs=[pl.BlockSpec((NR, 4, ROWS, LANES), lambda q, *_: (0, q, 0, 0))],
            out_specs=pl.BlockSpec((KX, N, LANES), lambda q, *_: (0, 0, q)),
            scratch_shapes=[pltpu.VMEM((4, LINED, LANES), jnp.float32)],
        ),
        out_shape=jax.ShapeDtypeStruct((KX, N, N), jnp.float32),
        name=name,
        cost_estimate=pl.CostEstimate(
            flops=2 * N * N * N * 4, bytes_accessed=2 * KX * N * N * 4, transcendentals=0
        ),
    )(starts, places, received.reshape(NR, NB, ROWS, LANES))


def slope_z_kernel(field_ref, high_ref, low_ref, out_ref):
    out_ref[0] = -mul3(halves(field_ref[0]), (high_ref[...], low_ref[...]))


def slope_y_kernel(field_ref, high_ref, low_ref, add_ref, out_ref):
    out_ref[0] = add_ref[0] + mul3((high_ref[...], low_ref[...]), halves(field_ref[0]))


def slopes(kernel, field, matrices, extra, name):
    block = pl.BlockSpec((1, N, N), lambda k: (k, 0, 0))
    whole = pl.BlockSpec((N, N), lambda k: (0, 0))
    return pl.pallas_call(
        kernel,
        grid=(KX,),
        in_specs=[block, whole, whole] + [block] * len(extra),
        out_specs=block,
        out_shape=jax.ShapeDtypeStruct((KX, N, N), jnp.float32),
        name=name,
        cost_estimate=pl.CostEstimate(
            flops=6 * KX * N * N * N, bytes_accessed=2 * KX * N * N * 4, transcendentals=0
        ),
    )(field, *matrices, *extra)


def finish_kernel(starts, places, in_ref, part_ref, sort_ref, out_ref, peak_ref, lined, total, top):
    quad = pl.program_id(0)
    gather_quad(starts, places, in_ref, lined, quad)

    def step(t, carry):
        rows = pl.ds(pl.multiple_of(t * CHUNK, CHUNK), CHUNK)
        turned = turn_lanes([lined[cc, rows, :] for cc in range(4)])
        for k in range(KX):
            total[k, rows, :] = turned[k] + part_ref[k, rows, :]
        return carry

    lax.fori_loop(0, N // CHUNK, step, 0)
    sorter = sort_ref[0]
    for k in range(KX):
        for m in range(2):
            low_rows = total[k, pl.ds(m * 256, LANES), :]
            high_rows = total[k, pl.ds(m * 256 + LANES, LANES), :]
            wide = jnp.concatenate([low_rows, high_rows], axis=1)
            first, second = halves(wide)
            dims = (((1,), (1,)), ((), ()))
            tall = lax.dot_general(
                sorter, first, dims, preferred_element_type=jnp.float32
            ) + lax.dot_general(sorter, second, dims, preferred_element_type=jnp.float32)
            tiles = tall.reshape(32, 8, LANES)
            at = (k * 2 + m) * 8
            out_ref[:, at : at + 8, :] = tiles
            best = jnp.max(jnp.abs(tiles), axis=0)

            @pl.when(quad == 0)
            def _():
                top[at : at + 8, :] = best

            @pl.when(quad != 0)
            def _():
                top[at : at + 8, :] = jnp.maximum(top[at : at + 8, :], best)

    @pl.when(quad == 3)
    def _():
        peak = top[pl.ds(0, 16, stride=4), :]
        for gp in range(1, 4):
            peak = jnp.maximum(peak, top[pl.ds(gp, 16, stride=4), :])
        peak_ref[...] = jnp.broadcast_to(peak[None], peak_ref.shape)


def finish(received, part, sorter, starts, places):
    return pl.pallas_call(
        finish_kernel,
        grid_spec=pltpu.PrefetchScalarGridSpec(
            num_scalar_prefetch=2,
            grid=(4,),
            in_specs=[
                pl.BlockSpec((NR, 4, ROWS, LANES), lambda q, *_: (0, q, 0, 0)),
                pl.BlockSpec((KX, N, LANES), lambda q, *_: (0, 0, q)),
                pl.BlockSpec((1, 256, 256), lambda q, *_: (q, 0, 0)),
            ],
            out_specs=[
                pl.BlockSpec((32, 64, LANES), lambda q, *_: (q, 0, 0)),
                pl.BlockSpec((DEVICES, 16, LANES), lambda q, *_: (0, 0, 0)),
            ],
            scratch_shapes=[
                pltpu.VMEM((4, LINED, LANES), jnp.float32),
                pltpu.VMEM((KX, N, LANES), jnp.float32),
                pltpu.VMEM((64, LANES), jnp.float32),
            ],
        ),
        out_shape=[
            jax.ShapeDtypeStruct((DEVICES, 64, LANES), jnp.float32),
            jax.ShapeDtypeStruct((DEVICES, 16, LANES), jnp.float32),
        ],
        name="finish",
        cost_estimate=pl.CostEstimate(
            flops=4 * N * N * N, bytes_accessed=4 * KX * N * N * 4, transcendentals=0
        ),
    )(starts, places, received.reshape(NR, NB, ROWS, LANES), part, sorter)


def sorters(new_col):
    block = jnp.arange(4, dtype=jnp.int32)
    device = (block // 2)[None, :, None] * 16 + new_col.reshape(4, 4, NB)
    slot = device * 8 + (block % 2)[None, :, None] * 2
    j = jnp.arange(2, dtype=jnp.int32)
    p = jnp.arange(2, dtype=jnp.int32)
    target = slot[:, None, :, :, None] + j[None, :, None, None, None] * 4 + p
    target = target.reshape(4, 1, 256)
    hit = target == jnp.arange(256, dtype=jnp.int32)[None, :, None]
    return hit.astype(jnp.bfloat16)


def unpack_slab_kernel(in_ref, out_ref):
    for j in range(2):
        for gp in range(4):
            out_ref[gp, j * LANES : (j + 1) * LANES, :] = in_ref[:, j * 4 + gp, :].T


def unpack_slab(arrived):
    return pl.pallas_call(
        unpack_slab_kernel,
        grid=(KX, 2),
        in_specs=[pl.BlockSpec((DEVICES, 8, LANES), lambda k, m: (0, k * 2 + m, 0))],
        out_specs=pl.BlockSpec((4, 256, LANES), lambda k, m: (0, m, k)),
        out_shape=jax.ShapeDtypeStruct((4, N, N), jnp.float32),
        name="unpack_slab",
    )(arrived)


def unpack_peak_kernel(in_ref, out_ref):
    for half in range(2):
        for y in range(4):
            out_ref[y * LANES : (y + 1) * LANES, half * LANES : (half + 1) * LANES] = in_ref[
                :, half * 4 + y, :
            ].T


def unpack_peak(arrived):
    return pl.pallas_call(
        unpack_peak_kernel,
        grid=(2,),
        in_specs=[pl.BlockSpec((DEVICES, 8, LANES), lambda t: (0, t, 0))],
        out_specs=pl.BlockSpec((N, 256), lambda t: (0, t)),
        out_shape=jax.ShapeDtypeStruct((N, N), jnp.float32),
        name="unpack_peak",
    )(arrived)


def exchange(value):
    return lax.all_to_all(value, AXES, split_axis=0, concat_axis=0, tiled=True)


def on_device(velocity, y_sizes, old_place, new_col):
    velocity = velocity.reshape(3, ROWS, ZB, N)
    starts = jnp.cumsum(y_sizes) - y_sizes
    matrices = tuple(jnp.asarray(part) for part in spectral_pair())
    sorter = sorters(new_col)
    got_2 = exchange(pack(velocity, 2))
    got_1 = exchange(pack(velocity, 1))
    got_0 = exchange(pack(velocity, 0, matrices))
    part = slopes(slope_z_kernel, gather(got_2, starts, old_place, "gather_2"), matrices, (), "slope_z")
    part = slopes(
        slope_y_kernel, gather(got_1, starts, old_place, "gather_1"), matrices, (part,), "slope_y"
    )
    packed, peaks = finish(got_0, part, sorter, starts, old_place)
    slab = unpack_slab(exchange(packed))
    peak = unpack_peak(exchange(peaks))
    return slab.reshape(2, 1, 2, N, N), peak


def solution(mesh):
    in_specs = (P(None, "col", "row", None, None, None), P(), P(), P())
    out_specs = (P("row", "col", None, None, None), P())
    return jax.shard_map(
        on_device, mesh=mesh, in_specs=in_specs, out_specs=out_specs, check_vma=False
    )
```

```python
import jax
import jax.numpy as jnp
import numpy as np
from jax import lax
from jax.experimental import pallas as pl
from jax.experimental.pallas import tpu as pltpu
from jax.sharding import PartitionSpec as P

AXES = ("col", "row")
LANES = 128
N = 512
DEVICES = 128
KX = N // DEVICES
ROWS = 72
CAP = 36
PLACED = 80
ZB = 32
NB = 16
NR = 8


def spectral_pair():
    gap = (np.arange(N)[:, None] - np.arange(N)[None, :]) % N
    angle = gap * (np.pi / N)
    parity = 1.0 - 2.0 * (gap % 2)
    safe = np.where(gap == 0, 1.0, np.sin(angle))
    full = np.where(gap == 0, 0.0, parity * np.cos(angle) / safe * (2.0 / N))
    full = (full - full.T) / 2
    high = full.astype(jnp.bfloat16)
    low = (full - high.astype(np.float64)).astype(jnp.bfloat16)
    return high, low


def halves(value):
    high = value.astype(jnp.bfloat16)
    return high, (value - high.astype(jnp.float32)).astype(jnp.bfloat16)


def mul(left, right):
    return jnp.dot(left, right, preferred_element_type=jnp.float32)


def mul3(left, right):
    return mul(left[0], right[0]) + (mul(left[1], right[0]) + mul(left[0], right[1]))


def pack_rows(value, out_ref, i):
    tall = jnp.concatenate([value[:, k * LANES : (k + 1) * LANES] for k in range(KX)], axis=0)
    out_ref[:, i, :] = tall.T


FIELDS = (2, 1)
STEPS = ROWS // 8


def pack_pair_kernel(in_ref, out_ref, taken, made, in_sem, out_sem):
    def load(step):
        field, t = divmod(step, STEPS)
        return pltpu.make_async_copy(
            in_ref.at[FIELDS[field], pl.ds(t * 8, 8)], taken.at[step], in_sem.at[step]
        )

    def store(step):
        return pltpu.make_async_copy(
            made.at[step], out_ref.at[:, pl.ds(step * 8, 8), :], out_sem.at[step]
        )

    total = STEPS * len(FIELDS)
    for step in range(total):
        load(step).start()
    for step in range(total):
        load(step).wait()
        for i in range(8):
            pack_rows(taken[step, i], made.at[step], i)
        store(step).start()
    for step in range(total):
        store(step).wait()


def pack_pair(velocity):
    total = STEPS * len(FIELDS)
    return pl.pallas_call(
        pack_pair_kernel,
        in_specs=[pl.BlockSpec(memory_space=pl.ANY)],
        out_specs=pl.BlockSpec(memory_space=pl.ANY),
        out_shape=jax.ShapeDtypeStruct((DEVICES, total * 8, LANES), jnp.float32),
        scratch_shapes=[
            pltpu.VMEM((total, 8, ZB, N), jnp.float32),
            pltpu.VMEM((total, DEVICES, 8, LANES), jnp.float32),
            pltpu.SemaphoreType.DMA((total,)),
            pltpu.SemaphoreType.DMA((total,)),
        ],
        name="pack_pair",
        cost_estimate=pl.CostEstimate(
            flops=2 * ROWS * ZB * N * N, bytes_accessed=4 * ROWS * ZB * N * 4, transcendentals=0
        ),
    )(velocity)


def pack_slope(in_ref, high_ref, low_ref, out_ref):
    flat = in_ref[0].reshape(8 * ZB, N)
    slope = -mul3(halves(flat), (high_ref[...], low_ref[...]))
    for i in range(8):
        pack_rows(slope[i * ZB : (i + 1) * ZB], out_ref, i)


def pack_derived(velocity, matrices):
    return pl.pallas_call(
        pack_slope,
        grid=(STEPS,),
        in_specs=[pl.BlockSpec((1, 8, ZB, N), lambda t: (0, t, 0, 0))]
        + [pl.BlockSpec((N, N), lambda t: (0, 0))] * 2,
        out_specs=pl.BlockSpec((DEVICES, 8, LANES), lambda t: (0, t, 0)),
        out_shape=jax.ShapeDtypeStruct((DEVICES, ROWS, LANES), jnp.float32),
        name="pack_slope",
        cost_estimate=pl.CostEstimate(
            flops=6 * ROWS * ZB * N * N, bytes_accessed=2 * ROWS * ZB * N * 4, transcendentals=0
        ),
    )(velocity, *matrices)


def gather_quad(starts, places, in_ref, lined, quad, first=0):
    for cc in range(4):
        for b in range(NB):
            place = places[quad * 4 + cc, b]
            source = in_ref[first + cc, place // 2, pl.ds((place % 2) * CAP, CAP), :]
            lined[cc, pl.ds(starts[b], CAP), :] = source


def turn_lanes(parts):
    lane = lax.broadcasted_iota(jnp.int32, parts[0].shape, 1)
    upper = (lane // 64) == 1
    odd = (lane // 32) % 2 == 1
    a0, a1, a2, a3 = parts
    b0 = jnp.where(upper, pltpu.roll(a2, 64, 1), a0)
    b2 = jnp.where(upper, a2, pltpu.roll(a0, 64, 1))
    b1 = jnp.where(upper, pltpu.roll(a3, 64, 1), a1)
    b3 = jnp.where(upper, a3, pltpu.roll(a1, 64, 1))
    c0 = jnp.where(odd, pltpu.roll(b1, 32, 1), b0)
    c1 = jnp.where(odd, b1, pltpu.roll(b0, 96, 1))
    c2 = jnp.where(odd, pltpu.roll(b3, 32, 1), b2)
    c3 = jnp.where(odd, b3, pltpu.roll(b2, 96, 1))
    return c0, c1, c2, c3


CHUNK = 64


def gather_kernel(starts, places, in_ref, out_ref, lined):
    gather_quad(starts, places, in_ref, lined, pl.program_id(0))

    def step(t, carry):
        rows = pl.ds(pl.multiple_of(t * CHUNK, CHUNK), CHUNK)
        turned = turn_lanes([lined[cc, rows, :] for cc in range(4)])
        for k in range(KX):
            out_ref[k, rows, :] = turned[k]
        return carry

    lax.fori_loop(0, N // CHUNK, step, 0)


LINED = 560


def gather(received, field, starts, places, name):
    return pl.pallas_call(
        gather_kernel,
        grid_spec=pltpu.PrefetchScalarGridSpec(
            num_scalar_prefetch=2,
            grid=(4,),
            in_specs=[pl.BlockSpec((4, NR, ROWS, LANES), lambda q, *_: (q, 0, field, 0))],
            out_specs=pl.BlockSpec((KX, N, LANES), lambda q, *_: (0, 0, q)),
            scratch_shapes=[pltpu.VMEM((4, LINED, LANES), jnp.float32)],
        ),
        out_shape=jax.ShapeDtypeStruct((KX, N, N), jnp.float32),
        name=name,
        cost_estimate=pl.CostEstimate(
            flops=2 * N * N * N * 4, bytes_accessed=2 * KX * N * N * 4, transcendentals=0
        ),
    )(starts, places, received.reshape(NB, NR, -1, LANES))


def slope_z_kernel(field_ref, high_ref, low_ref, out_ref):
    out_ref[0] = -mul3(halves(field_ref[0]), (high_ref[...], low_ref[...]))


def slope_y_kernel(field_ref, high_ref, low_ref, add_ref, out_ref):
    total = add_ref[0] + mul3((high_ref[...], low_ref[...]), halves(field_ref[0]))
    for quad in range(4):
        out_ref[quad, 0] = total[:, quad * LANES : (quad + 1) * LANES]


BLOCK = pl.BlockSpec((1, N, N), lambda k: (k, 0, 0))
WHOLE = pl.BlockSpec((N, N), lambda k: (0, 0))
COST = pl.CostEstimate(
    flops=6 * KX * N * N * N, bytes_accessed=2 * KX * N * N * 4, transcendentals=0
)


def slope_z(field, matrices):
    return pl.pallas_call(
        slope_z_kernel,
        grid=(KX,),
        in_specs=[BLOCK, WHOLE, WHOLE],
        out_specs=BLOCK,
        out_shape=jax.ShapeDtypeStruct((KX, N, N), jnp.float32),
        name="slope_z",
        cost_estimate=COST,
    )(field, *matrices)


def slope_y(field, matrices, other):
    return pl.pallas_call(
        slope_y_kernel,
        grid=(KX,),
        in_specs=[BLOCK, WHOLE, WHOLE, BLOCK],
        out_specs=pl.BlockSpec((4, 1, N, LANES), lambda k: (0, k, 0, 0)),
        out_shape=jax.ShapeDtypeStruct((4, KX, N, LANES), jnp.float32),
        name="slope_y",
        cost_estimate=COST,
    )(field, *matrices, other)


def finish_kernel(
    starts, places, order_ref, in_ref, part_ref, out_ref,
    taken, part, lined, total, made, top, spread, in_sem, part_sem, out_sem, peak_sem,
):
    def load(quad):
        return (
            pltpu.make_async_copy(
                in_ref.at[pl.ds(quad * 4, 4)], taken.at[pl.ds(quad * 4, 4)], in_sem.at[quad]
            ),
            pltpu.make_async_copy(part_ref.at[quad], part.at[quad], part_sem.at[quad]),
        )

    def store(quad, side):
        return pltpu.make_async_copy(
            made.at[quad, pl.ds(side * NB, NB), pl.ds(0, 64), :],
            out_ref.at[:, quad * 2 + side, pl.ds(0, 64), :],
            out_sem.at[quad, side],
        )

    for quad in range(4):
        for copy in load(quad):
            copy.start()
    top[...] = jnp.zeros_like(top)

    def one(quad, carry):
        for copy in load(quad):
            copy.wait()
        gather_quad(starts, places, taken, lined, quad, quad * 4)
        order = jnp.broadcast_to(order_ref[pl.ds(quad, 1), :], (CHUNK, LANES))

        def step(t, carry):
            rows = pl.ds(pl.multiple_of(t * CHUNK, CHUNK), CHUNK)
            turned = turn_lanes([lined[cc, rows, :] for cc in range(4)])
            for k in range(KX):
                value = turned[k] + part[quad, k, rows, :]
                total[k, rows, :] = jnp.take_along_axis(value, order, axis=1)
            return carry

        lax.fori_loop(0, N // CHUNK, step, 0)
        for k in range(KX):
            for yb in range(4):
                tile = total[k, yb * LANES : (yb + 1) * LANES, :].T
                at = k * 4 + yb
                for gp in range(4):
                    made[quad, :, at * 4 + gp, :] = tile[gp * 32 : (gp + 1) * 32, :]
                best = jnp.max(jnp.abs(tile).reshape(16, 8, LANES), axis=0)
                top[at * 8 : at * 8 + 8, :] = jnp.maximum(top[at * 8 : at * 8 + 8, :], best)
        for side in range(2):
            store(quad, side).start()
        return carry

    lax.fori_loop(0, 4, one, 0)
    peak = jnp.max(top[...].reshape(16, 8, LANES), axis=1)
    spread[...] = jnp.broadcast_to(peak[None, None], spread.shape)
    last = pltpu.make_async_copy(spread, out_ref.at[:, :, pl.ds(64, 16), :], peak_sem)
    last.start()
    for quad in range(4):
        for side in range(2):
            store(quad, side).wait()
    last.wait()


MADE = 72


def finish(received, part, order, starts, places):
    anywhere = pl.BlockSpec(memory_space=pl.ANY)
    return pl.pallas_call(
        finish_kernel,
        grid_spec=pltpu.PrefetchScalarGridSpec(
            num_scalar_prefetch=2,
            grid=(1,),
            in_specs=[pl.BlockSpec((4, LANES), lambda i, *_: (0, 0)), anywhere, anywhere],
            out_specs=anywhere,
            scratch_shapes=[
                pltpu.VMEM((NB, NR, ROWS, LANES), jnp.float32),
                pltpu.VMEM((4, KX, N, LANES), jnp.float32),
                pltpu.VMEM((4, LINED, LANES), jnp.float32),
                pltpu.VMEM((KX, N, LANES), jnp.float32),
                pltpu.VMEM((4, 32, MADE, LANES), jnp.float32),
                pltpu.VMEM((LANES, LANES), jnp.float32),
                pltpu.VMEM((NB, NR, 16, LANES), jnp.float32),
                pltpu.SemaphoreType.DMA((4,)),
                pltpu.SemaphoreType.DMA((4,)),
                pltpu.SemaphoreType.DMA((4, 2)),
                pltpu.SemaphoreType.DMA,
            ],
        ),
        out_shape=jax.ShapeDtypeStruct((NB, NR, PLACED, LANES), jnp.float32),
        name="finish",
        cost_estimate=pl.CostEstimate(
            flops=4 * N * N * N, bytes_accessed=4 * KX * N * N * 4, transcendentals=0
        ),
    )(starts, places, order, received.reshape(NB, NR, ROWS, LANES), part)


def lane_order(new_col):
    slab = jnp.arange(NB, dtype=jnp.int32)
    hits = (new_col[:, :, None] == slab[None, None, :]).astype(jnp.int32)
    slab_of = jnp.sum(hits * slab[None, :, None], axis=1).reshape(4, 2, 2, NB)
    block = jnp.arange(4, dtype=jnp.int32).reshape(1, 2, 2, 1)
    lane = block * ZB + slab_of * 2
    lane = jnp.swapaxes(lane, 1, 2)[:, :, None] + jnp.arange(2, dtype=jnp.int32)[:, None, None]
    return lane.reshape(4, LANES)


def unpack_kernel(in_ref, slab_ref, peak_ref, taken, slab, peak, in_sem, slab_sem, peak_sem):
    def load(t):
        return pltpu.make_async_copy(
            in_ref.at[:, pl.ds(t * 8, 8), :], taken.at[t], in_sem.at[t]
        )

    def store(t):
        k, m = divmod(t, 2)
        return pltpu.make_async_copy(
            slab.at[t],
            slab_ref.at[:, pl.ds(m * 256, 256), pl.ds(k * LANES, LANES)],
            slab_sem.at[t],
        )

    def store_peak(t):
        return pltpu.make_async_copy(
            peak.at[t], peak_ref.at[:, pl.ds(t * 256, 256)], peak_sem.at[t]
        )

    for t in range(10):
        load(t).start()
    for t in range(8):
        load(t).wait()
        for j in range(2):
            for gp in range(4):
                slab[t, gp, j * LANES : (j + 1) * LANES, :] = taken[t, :, j * 4 + gp, :].T
        store(t).start()
    for t in range(2):
        load(8 + t).wait()
        for half in range(2):
            for yb in range(4):
                peak[t, yb * LANES : (yb + 1) * LANES, half * LANES : (half + 1) * LANES] = (
                    taken[8 + t, :, half * 4 + yb, :].T
                )
        store_peak(t).start()
    for t in range(8):
        store(t).wait()
    for t in range(2):
        store_peak(t).wait()


def unpack(arrived):
    anywhere = pl.BlockSpec(memory_space=pl.ANY)
    return pl.pallas_call(
        unpack_kernel,
        in_specs=[anywhere],
        out_specs=[anywhere, anywhere],
        out_shape=[
            jax.ShapeDtypeStruct((4, N, N), jnp.float32),
            jax.ShapeDtypeStruct((N, N), jnp.float32),
        ],
        scratch_shapes=[
            pltpu.VMEM((10, DEVICES, 8, LANES), jnp.float32),
            pltpu.VMEM((8, 4, 256, LANES), jnp.float32),
            pltpu.VMEM((2, N, 256), jnp.float32),
            pltpu.SemaphoreType.DMA((10,)),
            pltpu.SemaphoreType.DMA((8,)),
            pltpu.SemaphoreType.DMA((2,)),
        ],
        name="unpack",
    )(arrived)


def exchange(value):
    return lax.all_to_all(value, AXES, split_axis=0, concat_axis=0, tiled=True)


def on_device(velocity, y_sizes, old_place, new_col):
    velocity = velocity.reshape(3, ROWS, ZB, N)
    starts = jnp.cumsum(y_sizes) - y_sizes
    matrices = tuple(jnp.asarray(part) for part in spectral_pair())
    order = lane_order(new_col)
    pair = exchange(pack_pair(velocity))
    derived = exchange(pack_derived(velocity, matrices))
    part = slope_z(gather(pair, 0, starts, old_place, "gather_2"), matrices)
    part = slope_y(gather(pair, 1, starts, old_place, "gather_1"), matrices, part)
    packed = finish(derived, part, order, starts, old_place)
    slab, peak = unpack(exchange(packed.reshape(DEVICES, PLACED, LANES)))
    return slab.reshape(2, 1, 2, N, N), peak


def solution(mesh):
    in_specs = (P(None, "col", "row", None, None, None), P(), P(), P())
    out_specs = (P("row", "col", None, None, None), P())
    return jax.shard_map(
        on_device, mesh=mesh, in_specs=in_specs, out_specs=out_specs, check_vma=False
    )
```

```python
import jax
import jax.numpy as jnp
import numpy as np
from jax import lax
from jax.experimental import pallas as pl
from jax.experimental.pallas import tpu as pltpu
from jax.sharding import PartitionSpec as P

AXES = ("col", "row")
LANES = 128
N = 512
DEVICES = 128
KX = N // DEVICES
ROWS = 72
CAP = 36
PLACED = 80
ZB = 32
NB = 16
NR = 8


def spectral_pair():
    gap = (np.arange(N)[:, None] - np.arange(N)[None, :]) % N
    angle = gap * (np.pi / N)
    parity = 1.0 - 2.0 * (gap % 2)
    safe = np.where(gap == 0, 1.0, np.sin(angle))
    full = np.where(gap == 0, 0.0, parity * np.cos(angle) / safe * (2.0 / N))
    full = (full - full.T) / 2
    high = full.astype(jnp.bfloat16)
    low = (full - high.astype(np.float64)).astype(jnp.bfloat16)
    return high, low


def halves(value):
    high = value.astype(jnp.bfloat16)
    return high, (value - high.astype(jnp.float32)).astype(jnp.bfloat16)


def mul(left, right):
    return jnp.dot(left, right, preferred_element_type=jnp.float32)


def mul3(left, right):
    return mul(left[0], right[0]) + (mul(left[1], right[0]) + mul(left[0], right[1]))


def pack_rows(value, out_ref, i):
    tall = jnp.concatenate([value[:, k * LANES : (k + 1) * LANES] for k in range(KX)], axis=0)
    out_ref[pl.ds(i, DEVICES, stride=8), :] = tall.T


FIELDS = (2, 1)
STEPS = ROWS // 8


def pack_pair_kernel(in_ref, out_ref, taken, made, in_sem, out_sem):
    def load(step):
        field, t = divmod(step, STEPS)
        return pltpu.make_async_copy(
            in_ref.at[FIELDS[field], pl.ds(t * 8, 8)], taken.at[step], in_sem.at[step]
        )

    def store(step):
        return pltpu.make_async_copy(
            made.at[step], out_ref.at[:, pl.ds(step * 8, 8), :], out_sem.at[step]
        )

    total = STEPS * len(FIELDS)
    for step in range(total):
        load(step).start()
    for step in range(total):
        load(step).wait()
        for i in range(8):
            pack_rows(taken[step, i], made.at[step].reshape(DEVICES * 8, LANES), i)
        store(step).start()
    for step in range(total):
        store(step).wait()


def pack_pair(velocity):
    total = STEPS * len(FIELDS)
    return pl.pallas_call(
        pack_pair_kernel,
        in_specs=[pl.BlockSpec(memory_space=pltpu.HBM)],
        out_specs=pl.BlockSpec(memory_space=pltpu.HBM),
        out_shape=jax.ShapeDtypeStruct((DEVICES, total * 8, LANES), jnp.float32),
        scratch_shapes=[
            pltpu.VMEM((total, 8, ZB, N), jnp.float32),
            pltpu.VMEM((total, DEVICES, 8, LANES), jnp.float32),
            pltpu.SemaphoreType.DMA((total,)),
            pltpu.SemaphoreType.DMA((total,)),
        ],
        name="pack_pair",
        cost_estimate=pl.CostEstimate(
            flops=2 * ROWS * ZB * N * N, bytes_accessed=4 * ROWS * ZB * N * 4, transcendentals=0
        ),
    )(velocity)


def pack_slope(in_ref, high_ref, low_ref, out_ref):
    flat = in_ref[0].reshape(8 * ZB, N)
    slope = -mul3(halves(flat), (high_ref[...], low_ref[...]))
    for i in range(8):
        pack_rows(slope[i * ZB : (i + 1) * ZB], out_ref.reshape(DEVICES * 8, LANES), i)


def pack_derived(velocity, matrices):
    return pl.pallas_call(
        pack_slope,
        grid=(STEPS,),
        in_specs=[pl.BlockSpec((1, 8, ZB, N), lambda t: (0, t, 0, 0))]
        + [pl.BlockSpec((N, N), lambda t: (0, 0))] * 2,
        out_specs=pl.BlockSpec((DEVICES, 8, LANES), lambda t: (0, t, 0)),
        out_shape=jax.ShapeDtypeStruct((DEVICES, ROWS, LANES), jnp.float32),
        name="pack_slope",
        cost_estimate=pl.CostEstimate(
            flops=6 * ROWS * ZB * N * N, bytes_accessed=2 * ROWS * ZB * N * 4, transcendentals=0
        ),
    )(velocity, *matrices)


def gather_quad(starts, places, in_ref, lined, quad, first=0):
    for cc in range(4):
        for b in range(NB):
            source = in_ref[first + cc, pl.ds(places[quad * 4 + cc, b], CAP), :]
            lined[cc, pl.ds(starts[b], CAP), :] = source


def turn_lanes(parts):
    lane = lax.broadcasted_iota(jnp.int32, parts[0].shape, 1)
    upper = (lane // 64) == 1
    odd = (lane // 32) % 2 == 1
    a0, a1, a2, a3 = parts
    b0 = jnp.where(upper, pltpu.roll(a2, 64, 1), a0)
    b2 = jnp.where(upper, a2, pltpu.roll(a0, 64, 1))
    b1 = jnp.where(upper, pltpu.roll(a3, 64, 1), a1)
    b3 = jnp.where(upper, a3, pltpu.roll(a1, 64, 1))
    c0 = jnp.where(odd, pltpu.roll(b1, 32, 1), b0)
    c1 = jnp.where(odd, b1, pltpu.roll(b0, 96, 1))
    c2 = jnp.where(odd, pltpu.roll(b3, 32, 1), b2)
    c3 = jnp.where(odd, b3, pltpu.roll(b2, 96, 1))
    return c0, c1, c2, c3


CHUNK = 512


def gather_kernel(starts, places, in_ref, out_ref, lined):
    flat = in_ref.reshape(4, NR * ROWS, LANES)
    gather_quad(starts, places, flat, lined, pl.program_id(0))

    def step(t, carry):
        rows = pl.ds(pl.multiple_of(t * CHUNK, CHUNK), CHUNK)
        turned = turn_lanes([lined[cc, rows, :] for cc in range(4)])
        for k in range(KX):
            out_ref[k, rows, :] = turned[k]
        return carry

    lax.fori_loop(0, N // CHUNK, step, 0)


LINED = 560


def gather(received, field, starts, places, name):
    return pl.pallas_call(
        gather_kernel,
        grid_spec=pltpu.PrefetchScalarGridSpec(
            num_scalar_prefetch=2,
            grid=(4,),
            in_specs=[pl.BlockSpec((4, NR, ROWS, LANES), lambda q, *_: (q, 0, field, 0))],
            out_specs=pl.BlockSpec((KX, N, LANES), lambda q, *_: (0, 0, q)),
            scratch_shapes=[pltpu.VMEM((4, LINED, LANES), jnp.float32)],
        ),
        out_shape=jax.ShapeDtypeStruct((KX, N, N), jnp.float32),
        name=name,
        cost_estimate=pl.CostEstimate(
            flops=2 * N * N * N * 4, bytes_accessed=2 * KX * N * N * 4, transcendentals=0
        ),
    )(starts, places, received.reshape(NB, NR, -1, LANES))


def slope_z_kernel(field_ref, high_ref, low_ref, out_ref):
    out_ref[0] = -mul3(halves(field_ref[0]), (high_ref[...], low_ref[...]))


def slope_y_kernel(field_ref, high_ref, low_ref, add_ref, out_ref):
    total = add_ref[0] + mul3((high_ref[...], low_ref[...]), halves(field_ref[0]))
    for quad in range(4):
        out_ref[quad, 0] = total[:, quad * LANES : (quad + 1) * LANES]


BLOCK = pl.BlockSpec((1, N, N), lambda k: (k, 0, 0))
WHOLE = pl.BlockSpec((N, N), lambda k: (0, 0))
COST = pl.CostEstimate(
    flops=6 * KX * N * N * N, bytes_accessed=2 * KX * N * N * 4, transcendentals=0
)


def slope_z(field, matrices):
    return pl.pallas_call(
        slope_z_kernel,
        grid=(KX,),
        in_specs=[BLOCK, WHOLE, WHOLE],
        out_specs=BLOCK,
        out_shape=jax.ShapeDtypeStruct((KX, N, N), jnp.float32),
        name="slope_z",
        cost_estimate=COST,
    )(field, *matrices)


def slope_y(field, matrices, other):
    return pl.pallas_call(
        slope_y_kernel,
        grid=(KX,),
        in_specs=[BLOCK, WHOLE, WHOLE, BLOCK],
        out_specs=pl.BlockSpec((4, 1, N, LANES), lambda k: (0, k, 0, 0)),
        out_shape=jax.ShapeDtypeStruct((4, KX, N, LANES), jnp.float32),
        name="slope_y",
        cost_estimate=COST,
    )(field, *matrices, other)


def finish_kernel(
    starts, places, order_ref, in_ref, part_ref, out_ref,
    taken, part, lined, total, made, top, spread, in_sem, part_sem, out_sem, peak_sem,
):
    def load(quad):
        return (
            pltpu.make_async_copy(
                in_ref.at[pl.ds(quad * 4, 4)], taken.at[pl.ds(quad * 4, 4)], in_sem.at[quad]
            ),
            pltpu.make_async_copy(part_ref.at[quad], part.at[quad], part_sem.at[quad]),
        )

    def store(quad, side):
        return pltpu.make_async_copy(
            made.at[quad, pl.ds(side * NB, NB), pl.ds(0, 64), :],
            out_ref.at[:, quad * 2 + side, pl.ds(0, 64), :],
            out_sem.at[quad, side],
        )

    for quad in range(4):
        for copy in load(quad):
            copy.start()
    top[...] = jnp.zeros_like(top)

    def one(quad, carry):
        for copy in load(quad):
            copy.wait()
        gather_quad(starts, places, taken.reshape(NB, NR * ROWS, LANES), lined, quad, quad * 4)
        order = jnp.broadcast_to(order_ref[pl.ds(quad, 1), :], (CHUNK, LANES))

        def step(t, carry):
            rows = pl.ds(pl.multiple_of(t * CHUNK, CHUNK), CHUNK)
            turned = turn_lanes([lined[cc, rows, :] for cc in range(4)])
            for k in range(KX):
                value = turned[k] + part[quad, k, rows, :]
                total[k, rows, :] = jnp.take_along_axis(value, order, axis=1)
            return carry

        lax.fori_loop(0, N // CHUNK, step, 0)
        for k in range(KX):
            for yb in range(4):
                tile = total[k, yb * LANES : (yb + 1) * LANES, :].T
                at = k * 4 + yb
                flat = made.at[quad].reshape(32 * MADE, LANES)
                for gp in range(4):
                    flat[pl.ds(at * 4 + gp, 32, stride=MADE), :] = tile[gp * 32 : (gp + 1) * 32, :]
                best = jnp.max(jnp.abs(tile).reshape(16, 8, LANES), axis=0)
                top[at * 8 : at * 8 + 8, :] = jnp.maximum(top[at * 8 : at * 8 + 8, :], best)
        for side in range(2):
            store(quad, side).start()
        return carry

    lax.fori_loop(0, 4, one, 0)
    peak = jnp.max(top[...].reshape(16, 8, LANES), axis=1)
    spread[...] = jnp.broadcast_to(peak[None, None], spread.shape)
    last = pltpu.make_async_copy(spread, out_ref.at[:, :, pl.ds(64, 16), :], peak_sem)
    last.start()
    for quad in range(4):
        for side in range(2):
            store(quad, side).wait()
    last.wait()


MADE = 72


def finish(received, part, order, starts, places):
    anywhere = pl.BlockSpec(memory_space=pl.ANY)
    far = pl.BlockSpec(memory_space=pltpu.HBM)
    return pl.pallas_call(
        finish_kernel,
        grid_spec=pltpu.PrefetchScalarGridSpec(
            num_scalar_prefetch=2,
            grid=(1,),
            in_specs=[pl.BlockSpec((4, LANES), lambda i, *_: (0, 0)), far, far],
            out_specs=anywhere,
            scratch_shapes=[
                pltpu.VMEM((NB, NR, ROWS, LANES), jnp.float32),
                pltpu.VMEM((4, KX, N, LANES), jnp.float32),
                pltpu.VMEM((4, LINED, LANES), jnp.float32),
                pltpu.VMEM((KX, N, LANES), jnp.float32),
                pltpu.VMEM((4, 32, MADE, LANES), jnp.float32),
                pltpu.VMEM((LANES, LANES), jnp.float32),
                pltpu.VMEM((NB, NR, 16, LANES), jnp.float32),
                pltpu.SemaphoreType.DMA((4,)),
                pltpu.SemaphoreType.DMA((4,)),
                pltpu.SemaphoreType.DMA((4, 2)),
                pltpu.SemaphoreType.DMA,
            ],
        ),
        out_shape=jax.ShapeDtypeStruct((NB, NR, PLACED, LANES), jnp.float32),
        name="finish",
        compiler_params=pltpu.CompilerParams(vmem_limit_bytes=57 << 20),
        cost_estimate=pl.CostEstimate(
            flops=4 * N * N * N, bytes_accessed=4 * KX * N * N * 4, transcendentals=0
        ),
    )(starts, places, order, received.reshape(NB, NR, ROWS, LANES), part)


def lane_order(new_col):
    slab = jnp.arange(NB, dtype=jnp.int32)
    hits = (new_col[:, :, None] == slab[None, None, :]).astype(jnp.int32)
    slab_of = jnp.sum(hits * slab[None, :, None], axis=1).reshape(4, 2, 2, NB)
    block = jnp.arange(4, dtype=jnp.int32).reshape(1, 2, 2, 1)
    lane = block * ZB + slab_of * 2
    lane = jnp.swapaxes(lane, 1, 2)[:, :, None] + jnp.arange(2, dtype=jnp.int32)[:, None, None]
    return lane.reshape(4, LANES)


def unpack_kernel(in_ref, slab_ref, peak_ref, taken, slab, peak, in_sem, slab_sem, peak_sem):
    def load(t):
        return pltpu.make_async_copy(
            in_ref.at[:, pl.ds(t * 8, 8), :], taken.at[t], in_sem.at[t]
        )

    def store(t):
        k, m = divmod(t, 2)
        return pltpu.make_async_copy(
            slab.at[t],
            slab_ref.at[:, pl.ds(m * 256, 256), pl.ds(k * LANES, LANES)],
            slab_sem.at[t],
        )

    def store_peak(t):
        return pltpu.make_async_copy(
            peak.at[t], peak_ref.at[:, pl.ds(t * 256, 256)], peak_sem.at[t]
        )

    def turn(t, row):
        flat = taken.at[t].reshape(DEVICES * 8, LANES)
        return flat[pl.ds(row, DEVICES, stride=8), :].T

    for t in range(10):
        load(t).start()
    for t in range(8):
        load(t).wait()
        for j in range(2):
            for gp in range(4):
                slab[t, gp, j * LANES : (j + 1) * LANES, :] = turn(t, j * 4 + gp)
        store(t).start()
    for t in range(2):
        load(8 + t).wait()
        for half in range(2):
            for yb in range(4):
                peak[t, yb * LANES : (yb + 1) * LANES, half * LANES : (half + 1) * LANES] = turn(
                    8 + t, half * 4 + yb
                )
        store_peak(t).start()
    for t in range(8):
        store(t).wait()
    for t in range(2):
        store_peak(t).wait()


def unpack(arrived):
    anywhere = pl.BlockSpec(memory_space=pl.ANY)
    return pl.pallas_call(
        unpack_kernel,
        in_specs=[anywhere],
        out_specs=[anywhere, anywhere],
        out_shape=[
            jax.ShapeDtypeStruct((4, N, N), jnp.float32),
            jax.ShapeDtypeStruct((N, N), jnp.float32),
        ],
        scratch_shapes=[
            pltpu.VMEM((10, DEVICES, 8, LANES), jnp.float32),
            pltpu.VMEM((8, 4, 256, LANES), jnp.float32),
            pltpu.VMEM((2, N, 256), jnp.float32),
            pltpu.SemaphoreType.DMA((10,)),
            pltpu.SemaphoreType.DMA((8,)),
            pltpu.SemaphoreType.DMA((2,)),
        ],
        name="unpack",
        compiler_params=pltpu.CompilerParams(vmem_limit_bytes=16 << 20),
    )(arrived)


def exchange(value):
    return lax.all_to_all(value, AXES, split_axis=0, concat_axis=0, tiled=True)


def on_device(velocity, y_sizes, old_place, new_col):
    velocity = velocity.reshape(3, ROWS, ZB, N)
    starts = jnp.cumsum(y_sizes) - y_sizes
    matrices = tuple(jnp.asarray(part) for part in spectral_pair())
    order = lane_order(new_col)
    first_row = old_place * CAP
    pair = exchange(pack_pair(velocity))
    derived = exchange(pack_derived(velocity, matrices))
    part = slope_z(gather(pair, 0, starts, first_row, "gather_2"), matrices)
    part = slope_y(gather(pair, 1, starts, first_row, "gather_1"), matrices, part)
    packed = finish(derived, part, order, starts, first_row)
    slab, peak = unpack(exchange(packed.reshape(DEVICES, PLACED, LANES)))
    return slab.reshape(2, 1, 2, N, N), peak


def solution(mesh):
    in_specs = (P(None, "col", "row", None, None, None), P(), P(), P())
    out_specs = (P("row", "col", None, None, None), P())
    return jax.shard_map(
        on_device, mesh=mesh, in_specs=in_specs, out_specs=out_specs, check_vma=False
    )
```

```python
import jax
import jax.numpy as jnp
import numpy as np
from jax import lax
from jax.experimental import pallas as pl
from jax.experimental.pallas import tpu as pltpu
from jax.sharding import PartitionSpec as P

AXES = ("col", "row")
LANES = 128
N = 512
DEVICES = 128
KX = N // DEVICES
ROWS = 72
CAP = 36
SENT = 3 * ROWS
PLACED = 80
ZB = 32
NB = 16
NR = 8
PACK_MIB = 44
MIDDLE_MIB = 26


def spectral_pair():
    gap = (np.arange(N)[:, None] - np.arange(N)[None, :]) % N
    angle = gap * (np.pi / N)
    parity = 1.0 - 2.0 * (gap % 2)
    safe = np.where(gap == 0, 1.0, np.sin(angle))
    full = np.where(gap == 0, 0.0, parity * np.cos(angle) / safe * (2.0 / N))
    full = (full - full.T) / 2
    high = full.astype(jnp.bfloat16)
    low = (full - high.astype(np.float64)).astype(jnp.bfloat16)
    return high, low


def halves(value):
    high = value.astype(jnp.bfloat16)
    return high, (value - high.astype(jnp.float32)).astype(jnp.bfloat16)


def mul(left, right):
    return jnp.dot(left, right, preferred_element_type=jnp.float32)


def mul3(left, right):
    return mul(left[0], right[0]) + (mul(left[1], right[0]) + mul(left[0], right[1]))


def pack_row(value, flat, row):
    tall = jnp.concatenate([value[:, k * LANES : (k + 1) * LANES] for k in range(KX)], axis=0)
    flat[pl.ds(row, DEVICES, stride=SENT), :] = tall.T


FIELDS = (2, 1, 0)
STEPS = ROWS // 8


def pack_kernel(in_ref, high_ref, low_ref, out_ref, taken, high, low, in_sem, sem):
    flat = out_ref.reshape(DEVICES * SENT, LANES)

    def load(step):
        field, t = divmod(step, STEPS)
        return pltpu.make_async_copy(
            in_ref.at[FIELDS[field], pl.ds(t * 8, 8)], taken.at[step], in_sem.at[step]
        )

    constants = (
        pltpu.make_async_copy(high_ref, high, sem.at[0]),
        pltpu.make_async_copy(low_ref, low, sem.at[1]),
    )
    for step in range(3 * STEPS):
        load(step).start()
        if step == STEPS:
            for copy in constants:
                copy.start()
    for copy in constants:
        copy.wait()
    for step in range(3 * STEPS):
        load(step).wait()
        value = taken[step].reshape(8 * ZB, N)
        if FIELDS[step // STEPS] == 0:
            value = -mul3(halves(value), (high[...], low[...]))
        for i in range(8):
            pack_row(value[i * ZB : (i + 1) * ZB], flat, step * 8 + i)


def pack(velocity, matrices):
    far = pl.BlockSpec(memory_space=pltpu.HBM)
    return pl.pallas_call(
        pack_kernel,
        in_specs=[far, far, far],
        out_specs=pl.BlockSpec(memory_space=pltpu.VMEM),
        out_shape=pltpu.VMEM((DEVICES, SENT, LANES), jnp.float32),
        scratch_shapes=[
            pltpu.VMEM((3 * STEPS, 8, ZB, N), jnp.float32),
            pltpu.VMEM((N, N), jnp.bfloat16),
            pltpu.VMEM((N, N), jnp.bfloat16),
            pltpu.SemaphoreType.DMA((3 * STEPS,)),
            pltpu.SemaphoreType.DMA((2,)),
        ],
        name="pack",
        compiler_params=pltpu.CompilerParams(vmem_limit_bytes=PACK_MIB << 20),
    )(velocity, *matrices)


def turn_lanes(parts):
    lane = lax.broadcasted_iota(jnp.int32, parts[0].shape, 1)
    upper = (lane // 64) == 1
    odd = (lane // 32) % 2 == 1
    a0, a1, a2, a3 = parts
    b0 = jnp.where(upper, pltpu.roll(a2, 64, 1), a0)
    b2 = jnp.where(upper, a2, pltpu.roll(a0, 64, 1))
    b1 = jnp.where(upper, pltpu.roll(a3, 64, 1), a1)
    b3 = jnp.where(upper, a3, pltpu.roll(a1, 64, 1))
    c0 = jnp.where(odd, pltpu.roll(b1, 32, 1), b0)
    c1 = jnp.where(odd, b1, pltpu.roll(b0, 96, 1))
    c2 = jnp.where(odd, pltpu.roll(b3, 32, 1), b2)
    c3 = jnp.where(odd, b3, pltpu.roll(b2, 96, 1))
    return c0, c1, c2, c3


LINED = 560
MADE = 72


def middle_kernel(
    sizes, places, columns, high_ref, low_ref, in_ref, out_ref,
    starts, first, high, low, lined, field_high, field_low, part, total, made, top, spread,
    sem, out_sem, peak_sem,
):
    constants = (
        pltpu.make_async_copy(high_ref, high, sem.at[0]),
        pltpu.make_async_copy(low_ref, low, sem.at[1]),
    )
    for copy in constants:
        copy.start()

    start = jnp.int32(0)
    for b in range(NB):
        starts[b] = start
        start = start + sizes[b]

    def rows_of(c, carry):
        for b in range(NB):
            place = places[c, b]
            first[c, b] = place * CAP + (place >> 1) * (SENT - ROWS)
        return carry

    lax.fori_loop(0, NB, rows_of, 0)
    flat = in_ref.reshape(NB, NR * SENT, LANES)

    def quad_of(field, quad):
        for cc in range(4):
            for b in range(NB):
                row = first[quad * 4 + cc, b] + field * ROWS
                lined[cc, pl.ds(starts[b], CAP), :] = flat[quad * 4 + cc, pl.ds(row, CAP), :]
        return turn_lanes([lined[cc, 0:N, :] for cc in range(4)])

    def store(quad, side):
        return pltpu.make_async_copy(
            made.at[quad, pl.ds(side * NB, NB), pl.ds(0, 64), :],
            out_ref.at[:, quad * 2 + side, pl.ds(0, 64), :],
            out_sem.at[quad, side],
        )

    def split_z(quad, carry):
        turned = quad_of(0, quad)
        for k in range(KX):
            field_high[k, quad], field_low[k, quad] = halves(turned[k])
        return carry

    lax.fori_loop(0, 4, split_z, 0)
    for copy in constants:
        copy.wait()

    def slope_z(k, carry):
        left = [
            jnp.concatenate([ref[k, quad] for quad in range(4)], axis=1)
            for ref in (field_high, field_low)
        ]
        slope = mul3(left, (high[...], low[...]))
        for quad in range(4):
            part[quad, k] = -slope[:, quad * LANES : (quad + 1) * LANES]
        return carry

    lax.fori_loop(0, KX, slope_z, 0)
    top[...] = jnp.zeros_like(top)
    lane = lax.broadcasted_iota(jnp.int32, (8, LANES), 1)
    lane_block = ((lane // NB) % 2) * 2 + lane // 64
    lane_column = lane % NB

    def one(quad, carry):
        wide = jnp.concatenate(quad_of(1, quad), axis=1)
        slope = mul3((high[...], low[...]), halves(wide))
        for k in range(KX):
            part[quad, k] = part[quad, k] + slope[:, k * LANES : (k + 1) * LANES]
        order = lane_block * ZB + (lane // 32) % 2
        for cc in range(4):
            for slab in range(NB):
                hit = (lane_block == cc) & (lane_column == columns[quad * 4 + cc, slab])
                order = order + jnp.where(hit, 2 * slab, 0)
        order = jnp.concatenate([order] * (N // 8), axis=0)
        turned = quad_of(2, quad)
        for k in range(KX):
            value = turned[k] + part[quad, k]
            total[k] = jnp.take_along_axis(value, order, axis=1)
        for k in range(KX):
            for yb in range(4):
                tile = total[k, yb * LANES : (yb + 1) * LANES, :].T
                at = k * 4 + yb
                rows = made.at[quad].reshape(32 * MADE, LANES)
                for gp in range(4):
                    rows[pl.ds(at * 4 + gp, 32, stride=MADE), :] = tile[gp * 32 : (gp + 1) * 32, :]
                best = jnp.max(jnp.abs(tile).reshape(16, 8, LANES), axis=0)
                top[at * 8 : at * 8 + 8, :] = jnp.maximum(top[at * 8 : at * 8 + 8, :], best)
        for side in range(2):
            store(quad, side).start()
        return carry

    lax.fori_loop(0, 4, one, 0)
    peak = jnp.max(top[...].reshape(16, 8, LANES), axis=1)
    spread[...] = jnp.broadcast_to(peak[None, None], spread.shape)
    last = pltpu.make_async_copy(spread, out_ref.at[:, :, pl.ds(64, 16), :], peak_sem)
    last.start()
    for quad in range(4):
        for side in range(2):
            store(quad, side).wait()
    last.wait()


def middle(received, matrices, y_sizes, old_place, new_col):
    anywhere = pl.BlockSpec(memory_space=pl.ANY)
    far = pl.BlockSpec(memory_space=pltpu.HBM)
    near = pl.BlockSpec(memory_space=pltpu.SMEM)
    return pl.pallas_call(
        middle_kernel,
        in_specs=[near, near, near, far, far, pl.BlockSpec(memory_space=pltpu.VMEM)],
        out_specs=anywhere,
        out_shape=pltpu.VMEM((NB, NR, PLACED, LANES), jnp.float32),
        scratch_shapes=[
            pltpu.SMEM((NB,), jnp.int32),
            pltpu.SMEM((NB, NB), jnp.int32),
            pltpu.VMEM((N, N), jnp.bfloat16),
            pltpu.VMEM((N, N), jnp.bfloat16),
            pltpu.VMEM((4, LINED, LANES), jnp.float32),
            pltpu.VMEM((KX, 4, N, LANES), jnp.bfloat16),
            pltpu.VMEM((KX, 4, N, LANES), jnp.bfloat16),
            pltpu.VMEM((4, KX, N, LANES), jnp.float32),
            pltpu.VMEM((KX, N, LANES), jnp.float32),
            pltpu.VMEM((4, 32, MADE, LANES), jnp.float32),
            pltpu.VMEM((LANES, LANES), jnp.float32),
            pltpu.VMEM((NB, NR, 16, LANES), jnp.float32),
            pltpu.SemaphoreType.DMA((2,)),
            pltpu.SemaphoreType.DMA((4, 2)),
            pltpu.SemaphoreType.DMA,
        ],
        name="middle",
        compiler_params=pltpu.CompilerParams(vmem_limit_bytes=MIDDLE_MIB << 20),
    )(y_sizes, old_place, new_col, *matrices, received.reshape(NB, NR, SENT, LANES))


def unpack_kernel(in_ref, slab_ref, peak_ref, taken, slab, peak, in_sem, slab_sem, peak_sem):
    def load(t):
        return pltpu.make_async_copy(
            in_ref.at[:, pl.ds(t * 8, 8), :], taken.at[t], in_sem.at[t]
        )

    def store(t):
        k, m = divmod(t, 2)
        return pltpu.make_async_copy(
            slab.at[t],
            slab_ref.at[:, pl.ds(m * 256, 256), pl.ds(k * LANES, LANES)],
            slab_sem.at[t],
        )

    def store_peak(t):
        return pltpu.make_async_copy(
            peak.at[t], peak_ref.at[:, pl.ds(t * 256, 256)], peak_sem.at[t]
        )

    def turn(t, row):
        flat = taken.at[t].reshape(DEVICES * 8, LANES)
        return flat[pl.ds(row, DEVICES, stride=8), :].T

    for t in range(10):
        load(t).start()
    for t in range(8):
        load(t).wait()
        for j in range(2):
            for gp in range(4):
                slab[t, gp, j * LANES : (j + 1) * LANES, :] = turn(t, j * 4 + gp)
        store(t).start()
    for t in range(2):
        load(8 + t).wait()
        for half in range(2):
            for yb in range(4):
                peak[t, yb * LANES : (yb + 1) * LANES, half * LANES : (half + 1) * LANES] = turn(
                    8 + t, half * 4 + yb
                )
        store_peak(t).start()
    for t in range(8):
        store(t).wait()
    for t in range(2):
        store_peak(t).wait()


def unpack(arrived):
    anywhere = pl.BlockSpec(memory_space=pl.ANY)
    return pl.pallas_call(
        unpack_kernel,
        in_specs=[anywhere],
        out_specs=[anywhere, anywhere],
        out_shape=[
            jax.ShapeDtypeStruct((4, N, N), jnp.float32),
            jax.ShapeDtypeStruct((N, N), jnp.float32),
        ],
        scratch_shapes=[
            pltpu.VMEM((10, DEVICES, 8, LANES), jnp.float32),
            pltpu.VMEM((8, 4, 256, LANES), jnp.float32),
            pltpu.VMEM((2, N, 256), jnp.float32),
            pltpu.SemaphoreType.DMA((10,)),
            pltpu.SemaphoreType.DMA((8,)),
            pltpu.SemaphoreType.DMA((2,)),
        ],
        name="unpack",
        compiler_params=pltpu.CompilerParams(vmem_limit_bytes=16 << 20),
    )(arrived)


def exchange(value):
    return lax.all_to_all(value, AXES, split_axis=0, concat_axis=0, tiled=True)


def on_device(velocity, y_sizes, old_place, new_col):
    matrices = tuple(jnp.asarray(part) for part in spectral_pair())
    received = exchange(pack(velocity.reshape(3, ROWS, ZB, N), matrices))
    packed = middle(received, matrices, y_sizes, old_place, new_col)
    slab, peak = unpack(exchange(packed.reshape(DEVICES, PLACED, LANES)))
    return slab.reshape(2, 1, 2, N, N), peak


def solution(mesh):
    in_specs = (P(None, "col", "row", None, None, None), P(), P(), P())
    out_specs = (P("row", "col", None, None, None), P())
    return jax.shard_map(
        on_device, mesh=mesh, in_specs=in_specs, out_specs=out_specs, check_vma=False
    )
```

```python
import jax
import jax.numpy as jnp
import numpy as np
from jax import lax
from jax.experimental import pallas as pl
from jax.experimental.pallas import tpu as pltpu
from jax.sharding import PartitionSpec as P

AXES = ("col", "row")
LANES = 128
N = 512
HALF = N // 2
DEVICES = 128
KX = N // DEVICES
ROWS = 72
CAP = 36
SENT = 3 * ROWS
PLACED = 80
ZB = 32
NB = 16
NR = 8
PACK_MIB = 44
MIDDLE_MIB = 26


def spectral_pair():
    gap = (np.arange(N)[:, None] - np.arange(N)[None, :]) % N
    angle = gap * (np.pi / N)
    parity = 1.0 - 2.0 * (gap % 2)
    safe = np.where(gap == 0, 1.0, np.sin(angle))
    full = np.where(gap == 0, 0.0, parity * np.cos(angle) / safe * (2.0 / N))
    full = (full - full.T) / 2
    first, second = full[:HALF, :HALF], full[:HALF, HALF:]
    both = np.concatenate([(first + second) / 2, (first - second) / 2], axis=0)
    high = both.astype(jnp.bfloat16)
    low = (both - high.astype(np.float64)).astype(jnp.bfloat16)
    return high, low


def halves(value):
    high = value.astype(jnp.bfloat16)
    return high, (value - high.astype(jnp.float32)).astype(jnp.bfloat16)


def mul(left, right):
    return jnp.dot(left, right, preferred_element_type=jnp.float32)


def mul3(left, right):
    return mul(left[0], right[0]) + (mul(left[1], right[0]) + mul(left[0], right[1]))


def parts_of(high, low):
    return (high[:HALF], low[:HALF]), (high[HALF:], low[HALF:])


def derive_lanes(value, high, low):
    even, odd = parts_of(high, low)
    left, right = value[:, :HALF], value[:, HALF:]
    from_sum = mul3(halves(left + right), even)
    from_difference = mul3(halves(left - right), odd)
    return jnp.concatenate([-(from_sum + from_difference), from_difference - from_sum], axis=1)


def derive_rows(value, high, low):
    even, odd = parts_of(high, low)
    top, bottom = value[:HALF], value[HALF:]
    from_sum = mul3(even, halves(top + bottom))
    from_difference = mul3(odd, halves(top - bottom))
    return jnp.concatenate([from_sum + from_difference, from_sum - from_difference], axis=0)


def pack_row(value, flat, row):
    tall = jnp.concatenate([value[:, k * LANES : (k + 1) * LANES] for k in range(KX)], axis=0)
    flat[pl.ds(row, DEVICES, stride=SENT), :] = tall.T


FIELDS = (2, 1, 0)
STEPS = ROWS // 8
GROUP = 3


def pack_kernel(in_ref, high_ref, low_ref, out_ref, taken, high, low, in_sem, sem):
    flat = out_ref.reshape(DEVICES * SENT, LANES)

    def load(step):
        field, t = divmod(step, STEPS)
        return pltpu.make_async_copy(
            in_ref.at[FIELDS[field], pl.ds(t * 8, 8)], taken.at[step], in_sem.at[step]
        )

    constants = (
        pltpu.make_async_copy(high_ref, high, sem.at[0]),
        pltpu.make_async_copy(low_ref, low, sem.at[1]),
    )
    for step in range(3 * STEPS):
        load(step).start()
    for copy in constants:
        copy.start()
    for step in range(2 * STEPS):
        load(step).wait()
        for i in range(8):
            pack_row(taken[step, i], flat, step * 8 + i)
    for copy in constants:
        copy.wait()
    for group in range(2 * STEPS, 3 * STEPS, GROUP):
        for step in range(group, group + GROUP):
            load(step).wait()
        lines = taken[group : group + GROUP].reshape(GROUP * 8 * ZB, N)
        slope = derive_lanes(lines, high[...], low[...])
        for i in range(GROUP * 8):
            pack_row(slope[i * ZB : (i + 1) * ZB], flat, group * 8 + i)


def pack(velocity, matrices):
    far = pl.BlockSpec(memory_space=pltpu.HBM)
    return pl.pallas_call(
        pack_kernel,
        in_specs=[far, far, far],
        out_specs=pl.BlockSpec(memory_space=pltpu.VMEM),
        out_shape=pltpu.VMEM((DEVICES, SENT, LANES), jnp.float32),
        scratch_shapes=[
            pltpu.VMEM((3 * STEPS, 8, ZB, N), jnp.float32),
            pltpu.VMEM((N, HALF), jnp.bfloat16),
            pltpu.VMEM((N, HALF), jnp.bfloat16),
            pltpu.SemaphoreType.DMA((3 * STEPS,)),
            pltpu.SemaphoreType.DMA((2,)),
        ],
        name="pack",
        compiler_params=pltpu.CompilerParams(vmem_limit_bytes=PACK_MIB << 20),
    )(velocity, *matrices)


def turn_lanes(parts):
    lane = lax.broadcasted_iota(jnp.int32, parts[0].shape, 1)
    upper = (lane // 64) == 1
    odd = (lane // 32) % 2 == 1
    a0, a1, a2, a3 = parts
    b0 = jnp.where(upper, pltpu.roll(a2, 64, 1), a0)
    b2 = jnp.where(upper, a2, pltpu.roll(a0, 64, 1))
    b1 = jnp.where(upper, pltpu.roll(a3, 64, 1), a1)
    b3 = jnp.where(upper, a3, pltpu.roll(a1, 64, 1))
    c0 = jnp.where(odd, pltpu.roll(b1, 32, 1), b0)
    c1 = jnp.where(odd, b1, pltpu.roll(b0, 96, 1))
    c2 = jnp.where(odd, pltpu.roll(b3, 32, 1), b2)
    c3 = jnp.where(odd, b3, pltpu.roll(b2, 96, 1))
    return c0, c1, c2, c3


LINED = 560
CHUNK = 128
MADE = 72


def middle_kernel(
    sizes, places, columns, high_ref, low_ref, in_ref, out_ref,
    starts, first, high, low, lined, field, part, slope_y, total, made, top, spread,
    sem, out_sem, peak_sem,
):
    constants = (
        pltpu.make_async_copy(high_ref, high, sem.at[0]),
        pltpu.make_async_copy(low_ref, low, sem.at[1]),
    )
    for copy in constants:
        copy.start()

    start = jnp.int32(0)
    for b in range(NB):
        starts[b] = start
        start = start + sizes[b]

    def rows_of(c, carry):
        for b in range(NB):
            place = places[c, b]
            first[c, b] = place * CAP + (place >> 1) * (SENT - ROWS)
        return carry

    lax.fori_loop(0, NB, rows_of, 0)
    flat = in_ref.reshape(NB, NR * SENT, LANES)

    def line_up(item, quad):
        for cc in range(4):
            for b in range(NB):
                row = first[quad * 4 + cc, b] + item * ROWS
                lined[cc, pl.ds(starts[b], CAP), :] = flat[quad * 4 + cc, pl.ds(row, CAP), :]

    def store(quad, side):
        return pltpu.make_async_copy(
            made.at[quad, pl.ds(side * NB, NB), pl.ds(0, 64), :],
            out_ref.at[:, quad * 2 + side, pl.ds(0, 64), :],
            out_sem.at[quad, side],
        )

    def split_z(quad, carry):
        line_up(0, quad)
        turned = turn_lanes([lined[cc, 0:N, :] for cc in range(4)])
        for k in range(KX):
            field[k, quad] = turned[k]
        return carry

    lax.fori_loop(0, 4, split_z, 0)
    for copy in constants:
        copy.wait()

    def slope_z(k, carry):
        line = jnp.concatenate([field[k, quad] for quad in range(4)], axis=1)
        slope = derive_lanes(line, high[...], low[...])
        for quad in range(4):
            part[quad, k] = slope[:, quad * LANES : (quad + 1) * LANES]
        return carry

    lax.fori_loop(0, KX, slope_z, 0)
    top[...] = jnp.zeros_like(top)
    lane = lax.broadcasted_iota(jnp.int32, (8, LANES), 1)
    lane_block = ((lane // NB) % 2) * 2 + lane // 64
    lane_column = lane % NB

    def one(quad, carry):
        line_up(1, quad)
        wide = jnp.concatenate([lined[cc, 0:N, :] for cc in range(4)], axis=1)
        slope = derive_rows(wide, high[...], low[...])
        for cc in range(4):
            slope_y[cc] = slope[:, cc * LANES : (cc + 1) * LANES]
        order = lane_block * ZB + (lane // 32) % 2
        for cc in range(4):
            for slab in range(NB):
                hit = (lane_block == cc) & (lane_column == columns[quad * 4 + cc, slab])
                order = order + jnp.where(hit, 2 * slab, 0)
        order = jnp.concatenate([order] * (CHUNK // 8), axis=0)
        line_up(2, quad)
        for at in range(0, N, CHUNK):
            rows = slice(at, at + CHUNK)
            turned = turn_lanes([slope_y[cc, rows, :] + lined[cc, rows, :] for cc in range(4)])
            for k in range(KX):
                value = turned[k] + part[quad, k, rows, :]
                total[k, rows, :] = jnp.take_along_axis(value, order, axis=1)
        for k in range(KX):
            for yb in range(4):
                tile = total[k, yb * LANES : (yb + 1) * LANES, :].T
                at = k * 4 + yb
                rows = made.at[quad].reshape(32 * MADE, LANES)
                for gp in range(4):
                    rows[pl.ds(at * 4 + gp, 32, stride=MADE), :] = tile[gp * 32 : (gp + 1) * 32, :]
                best = jnp.max(jnp.abs(tile).reshape(16, 8, LANES), axis=0)
                top[at * 8 : at * 8 + 8, :] = jnp.maximum(top[at * 8 : at * 8 + 8, :], best)
        for side in range(2):
            store(quad, side).start()
        return carry

    lax.fori_loop(0, 4, one, 0)
    peak = jnp.max(top[...].reshape(16, 8, LANES), axis=1)
    spread[...] = jnp.broadcast_to(peak[None, None], spread.shape)
    last = pltpu.make_async_copy(spread, out_ref.at[:, :, pl.ds(64, 16), :], peak_sem)
    last.start()
    for quad in range(4):
        for side in range(2):
            store(quad, side).wait()
    last.wait()


def middle(received, matrices, y_sizes, old_place, new_col):
    anywhere = pl.BlockSpec(memory_space=pl.ANY)
    far = pl.BlockSpec(memory_space=pltpu.HBM)
    near = pl.BlockSpec(memory_space=pltpu.SMEM)
    return pl.pallas_call(
        middle_kernel,
        in_specs=[near, near, near, far, far, pl.BlockSpec(memory_space=pltpu.VMEM)],
        out_specs=anywhere,
        out_shape=pltpu.VMEM((NB, NR, PLACED, LANES), jnp.float32),
        scratch_shapes=[
            pltpu.SMEM((NB,), jnp.int32),
            pltpu.SMEM((NB, NB), jnp.int32),
            pltpu.VMEM((N, HALF), jnp.bfloat16),
            pltpu.VMEM((N, HALF), jnp.bfloat16),
            pltpu.VMEM((4, LINED, LANES), jnp.float32),
            pltpu.VMEM((KX, 4, N, LANES), jnp.float32),
            pltpu.VMEM((4, KX, N, LANES), jnp.float32),
            pltpu.VMEM((4, N, LANES), jnp.float32),
            pltpu.VMEM((KX, N, LANES), jnp.float32),
            pltpu.VMEM((4, 32, MADE, LANES), jnp.float32),
            pltpu.VMEM((LANES, LANES), jnp.float32),
            pltpu.VMEM((NB, NR, 16, LANES), jnp.float32),
            pltpu.SemaphoreType.DMA((2,)),
            pltpu.SemaphoreType.DMA((4, 2)),
            pltpu.SemaphoreType.DMA,
        ],
        name="middle",
        compiler_params=pltpu.CompilerParams(vmem_limit_bytes=MIDDLE_MIB << 20),
    )(y_sizes, old_place, new_col, *matrices, received.reshape(NB, NR, SENT, LANES))


def unpack_kernel(in_ref, slab_ref, peak_ref, taken, slab, peak, in_sem, slab_sem, peak_sem):
    def load(t):
        return pltpu.make_async_copy(
            in_ref.at[:, pl.ds(t * 8, 8), :], taken.at[t], in_sem.at[t]
        )

    def store(t):
        k, m = divmod(t, 2)
        return pltpu.make_async_copy(
            slab.at[t],
            slab_ref.at[:, pl.ds(m * 256, 256), pl.ds(k * LANES, LANES)],
            slab_sem.at[t],
        )

    def store_peak(t):
        return pltpu.make_async_copy(
            peak.at[t], peak_ref.at[:, pl.ds(t * 256, 256)], peak_sem.at[t]
        )

    def turn(t, row):
        flat = taken.at[t].reshape(DEVICES * 8, LANES)
        return flat[pl.ds(row, DEVICES, stride=8), :].T

    for t in range(10):
        load(t).start()
    for t in range(8):
        load(t).wait()
        for j in range(2):
            for gp in range(4):
                slab[t, gp, j * LANES : (j + 1) * LANES, :] = turn(t, j * 4 + gp)
        store(t).start()
    for t in range(2):
        load(8 + t).wait()
        for half in range(2):
            for yb in range(4):
                peak[t, yb * LANES : (yb + 1) * LANES, half * LANES : (half + 1) * LANES] = turn(
                    8 + t, half * 4 + yb
                )
        store_peak(t).start()
    for t in range(8):
        store(t).wait()
    for t in range(2):
        store_peak(t).wait()


def unpack(arrived):
    anywhere = pl.BlockSpec(memory_space=pl.ANY)
    return pl.pallas_call(
        unpack_kernel,
        in_specs=[anywhere],
        out_specs=[anywhere, anywhere],
        out_shape=[
            jax.ShapeDtypeStruct((4, N, N), jnp.float32),
            jax.ShapeDtypeStruct((N, N), jnp.float32),
        ],
        scratch_shapes=[
            pltpu.VMEM((10, DEVICES, 8, LANES), jnp.float32),
            pltpu.VMEM((8, 4, 256, LANES), jnp.float32),
            pltpu.VMEM((2, N, 256), jnp.float32),
            pltpu.SemaphoreType.DMA((10,)),
            pltpu.SemaphoreType.DMA((8,)),
            pltpu.SemaphoreType.DMA((2,)),
        ],
        name="unpack",
        compiler_params=pltpu.CompilerParams(vmem_limit_bytes=16 << 20),
    )(arrived)


def exchange(value):
    return lax.all_to_all(value, AXES, split_axis=0, concat_axis=0, tiled=True)


def on_device(velocity, y_sizes, old_place, new_col):
    matrices = tuple(jnp.asarray(part) for part in spectral_pair())
    received = exchange(pack(velocity.reshape(3, ROWS, ZB, N), matrices))
    packed = middle(received, matrices, y_sizes, old_place, new_col)
    slab, peak = unpack(exchange(packed.reshape(DEVICES, PLACED, LANES)))
    return slab.reshape(2, 1, 2, N, N), peak


def solution(mesh):
    in_specs = (P(None, "col", "row", None, None, None), P(), P(), P())
    out_specs = (P("row", "col", None, None, None), P())
    return jax.shard_map(
        on_device, mesh=mesh, in_specs=in_specs, out_specs=out_specs, check_vma=False
    )
```

```python
import jax
import jax.numpy as jnp
import numpy as np
from jax import lax
from jax.experimental import pallas as pl
from jax.experimental.pallas import tpu as pltpu
from jax.sharding import PartitionSpec as P

AXES = ("col", "row")
LANES = 128
N = 512
HALF = N // 2
DEVICES = 128
KX = N // DEVICES
ROWS = 72
CAP = 36
SENT = 3 * ROWS
PLACED = 72
ZB = 32
NB = 16
NR = 8
PACK_MIB = 44
MIDDLE_MIB = 26


def spectral_pair():
    gap = (np.arange(N)[:, None] - np.arange(N)[None, :]) % N
    angle = gap * (np.pi / N)
    parity = 1.0 - 2.0 * (gap % 2)
    safe = np.where(gap == 0, 1.0, np.sin(angle))
    full = np.where(gap == 0, 0.0, parity * np.cos(angle) / safe * (2.0 / N))
    full = (full - full.T) / 2
    first, second = full[:HALF, :HALF], full[:HALF, HALF:]
    both = np.concatenate([(first + second) / 2, (first - second) / 2], axis=0)
    high = both.astype(jnp.bfloat16)
    low = (both - high.astype(np.float64)).astype(jnp.bfloat16)
    return high, low


def halves(value):
    high = value.astype(jnp.bfloat16)
    return high, (value - high.astype(jnp.float32)).astype(jnp.bfloat16)


def mul(left, right):
    return jnp.dot(left, right, preferred_element_type=jnp.float32)


def mul3(left, right):
    return mul(left[0], right[0]) + (mul(left[1], right[0]) + mul(left[0], right[1]))


def parts_of(high, low):
    return (high[:HALF], low[:HALF]), (high[HALF:], low[HALF:])


def derive_lanes(value, high, low):
    even, odd = parts_of(high, low)
    left, right = value[:, :HALF], value[:, HALF:]
    from_sum = mul3(halves(left + right), even)
    from_difference = mul3(halves(left - right), odd)
    return jnp.concatenate([-(from_sum + from_difference), from_difference - from_sum], axis=1)


def derive_rows(value, high, low):
    even, odd = parts_of(high, low)
    top, bottom = value[:HALF], value[HALF:]
    from_sum = mul3(even, halves(top + bottom))
    from_difference = mul3(odd, halves(top - bottom))
    return jnp.concatenate([from_sum + from_difference, from_sum - from_difference], axis=0)


def pack_row(value, flat, row):
    tall = jnp.concatenate([value[:, k * LANES : (k + 1) * LANES] for k in range(KX)], axis=0)
    flat[pl.ds(row, DEVICES, stride=SENT), :] = tall.T


FIELDS = (2, 1, 0)
STEPS = ROWS // 8
GROUP = 3


def pack_kernel(in_ref, high_ref, low_ref, out_ref, taken, high, low, in_sem, sem):
    flat = out_ref.reshape(DEVICES * SENT, LANES)

    def load(step):
        field, t = divmod(step, STEPS)
        return pltpu.make_async_copy(
            in_ref.at[FIELDS[field], pl.ds(t * 8, 8)], taken.at[step], in_sem.at[step]
        )

    constants = (
        pltpu.make_async_copy(high_ref, high, sem.at[0]),
        pltpu.make_async_copy(low_ref, low, sem.at[1]),
    )
    for step in range(3 * STEPS):
        load(step).start()
    for copy in constants:
        copy.start()
    for step in range(2 * STEPS):
        load(step).wait()
        for i in range(8):
            pack_row(taken[step, i], flat, step * 8 + i)
    for copy in constants:
        copy.wait()
    for group in range(2 * STEPS, 3 * STEPS, GROUP):
        for step in range(group, group + GROUP):
            load(step).wait()
        lines = taken[group : group + GROUP].reshape(GROUP * 8 * ZB, N)
        slope = derive_lanes(lines, high[...], low[...])
        for i in range(GROUP * 8):
            pack_row(slope[i * ZB : (i + 1) * ZB], flat, group * 8 + i)


def pack(velocity, matrices):
    far = pl.BlockSpec(memory_space=pltpu.HBM)
    return pl.pallas_call(
        pack_kernel,
        in_specs=[far, far, far],
        out_specs=pl.BlockSpec(memory_space=pltpu.VMEM),
        out_shape=pltpu.VMEM((DEVICES, SENT, LANES), jnp.float32),
        scratch_shapes=[
            pltpu.VMEM((3 * STEPS, 8, ZB, N), jnp.float32),
            pltpu.VMEM((N, HALF), jnp.bfloat16),
            pltpu.VMEM((N, HALF), jnp.bfloat16),
            pltpu.SemaphoreType.DMA((3 * STEPS,)),
            pltpu.SemaphoreType.DMA((2,)),
        ],
        name="pack",
        compiler_params=pltpu.CompilerParams(vmem_limit_bytes=PACK_MIB << 20),
    )(velocity, *matrices)


def turn_lanes(parts):
    lane = lax.broadcasted_iota(jnp.int32, parts[0].shape, 1)
    upper = (lane // 64) == 1
    odd = (lane // 32) % 2 == 1
    a0, a1, a2, a3 = parts
    b0 = jnp.where(upper, pltpu.roll(a2, 64, 1), a0)
    b2 = jnp.where(upper, a2, pltpu.roll(a0, 64, 1))
    b1 = jnp.where(upper, pltpu.roll(a3, 64, 1), a1)
    b3 = jnp.where(upper, a3, pltpu.roll(a1, 64, 1))
    c0 = jnp.where(odd, pltpu.roll(b1, 32, 1), b0)
    c1 = jnp.where(odd, b1, pltpu.roll(b0, 96, 1))
    c2 = jnp.where(odd, pltpu.roll(b3, 32, 1), b2)
    c3 = jnp.where(odd, b3, pltpu.roll(b2, 96, 1))
    return c0, c1, c2, c3


LINED = 560
CHUNK = 128
MADE = 72


def middle_kernel(
    sizes, places, columns, high_ref, low_ref, in_ref, out_ref,
    starts, first, high, low, lined, field, part, slope_y, total, made, top, spread,
    sem, out_sem, peak_sem,
):
    constants = (
        pltpu.make_async_copy(high_ref, high, sem.at[0]),
        pltpu.make_async_copy(low_ref, low, sem.at[1]),
    )
    for copy in constants:
        copy.start()

    start = jnp.int32(0)
    for b in range(NB):
        starts[b] = start
        start = start + sizes[b]

    def rows_of(c, carry):
        for b in range(NB):
            place = places[c, b]
            first[c, b] = place * CAP + (place >> 1) * (SENT - ROWS)
        return carry

    lax.fori_loop(0, NB, rows_of, 0)
    flat = in_ref.reshape(NB, NR * SENT, LANES)

    def line_up(item, quad):
        for cc in range(4):
            for b in range(NB):
                row = first[quad * 4 + cc, b] + item * ROWS
                lined[cc, pl.ds(starts[b], CAP), :] = flat[quad * 4 + cc, pl.ds(row, CAP), :]

    def store(quad, side):
        return pltpu.make_async_copy(
            made.at[quad, pl.ds(side * NB, NB), pl.ds(0, 64), :],
            out_ref.at[:, quad * 2 + side, pl.ds(0, 64), :],
            out_sem.at[quad, side],
        )

    def split_z(quad, carry):
        line_up(0, quad)
        turned = turn_lanes([lined[cc, 0:N, :] for cc in range(4)])
        for k in range(KX):
            field[k, quad] = turned[k]
        return carry

    lax.fori_loop(0, 4, split_z, 0)
    for copy in constants:
        copy.wait()

    def slope_z(k, carry):
        line = jnp.concatenate([field[k, quad] for quad in range(4)], axis=1)
        slope = derive_lanes(line, high[...], low[...])
        for quad in range(4):
            part[quad, k] = slope[:, quad * LANES : (quad + 1) * LANES]
        return carry

    lax.fori_loop(0, KX, slope_z, 0)
    top[...] = jnp.zeros_like(top)
    lane = lax.broadcasted_iota(jnp.int32, (8, LANES), 1)
    lane_block = ((lane // NB) % 2) * 2 + lane // 64
    lane_column = lane % NB

    def one(quad, carry):
        line_up(1, quad)
        wide = jnp.concatenate([lined[cc, 0:N, :] for cc in range(4)], axis=1)
        slope = derive_rows(wide, high[...], low[...])
        for cc in range(4):
            slope_y[cc] = slope[:, cc * LANES : (cc + 1) * LANES]
        order = lane_block * ZB + (lane // 32) % 2
        for cc in range(4):
            for slab in range(NB):
                hit = (lane_block == cc) & (lane_column == columns[quad * 4 + cc, slab])
                order = order + jnp.where(hit, 2 * slab, 0)
        order = jnp.concatenate([order] * (CHUNK // 8), axis=0)
        line_up(2, quad)
        for at in range(0, N, CHUNK):
            rows = slice(at, at + CHUNK)
            turned = turn_lanes([slope_y[cc, rows, :] + lined[cc, rows, :] for cc in range(4)])
            for k in range(KX):
                value = turned[k] + part[quad, k, rows, :]
                total[k, rows, :] = jnp.take_along_axis(value, order, axis=1)
        for k in range(KX):
            for yb in range(4):
                tile = total[k, yb * LANES : (yb + 1) * LANES, :].T
                at = k * 4 + yb
                rows = made.at[quad].reshape(32 * MADE, LANES)
                for gp in range(4):
                    rows[pl.ds(at * 4 + gp, 32, stride=MADE), :] = tile[gp * 32 : (gp + 1) * 32, :]
                best = jnp.max(jnp.abs(tile).reshape(16, 8, LANES), axis=0)
                top[at * 8 : at * 8 + 8, :] = jnp.maximum(top[at * 8 : at * 8 + 8, :], best)
        for side in range(2):
            store(quad, side).start()
        return carry

    lax.fori_loop(0, 4, one, 0)
    peak = jnp.max(top[...].reshape(16, 8, LANES), axis=1)
    for column in range(NB):
        half = peak[:8] if column % 2 == 0 else peak[8:]
        spread[column] = jnp.broadcast_to(half[None], (NR, 8, LANES))
    last = pltpu.make_async_copy(spread, out_ref.at[:, :, pl.ds(64, 8), :], peak_sem)
    last.start()
    for quad in range(4):
        for side in range(2):
            store(quad, side).wait()
    last.wait()


def middle(received, matrices, y_sizes, old_place, new_col):
    anywhere = pl.BlockSpec(memory_space=pl.ANY)
    far = pl.BlockSpec(memory_space=pltpu.HBM)
    near = pl.BlockSpec(memory_space=pltpu.SMEM)
    return pl.pallas_call(
        middle_kernel,
        in_specs=[near, near, near, far, far, pl.BlockSpec(memory_space=pltpu.VMEM)],
        out_specs=anywhere,
        out_shape=pltpu.VMEM((NB, NR, PLACED, LANES), jnp.float32),
        scratch_shapes=[
            pltpu.SMEM((NB,), jnp.int32),
            pltpu.SMEM((NB, NB), jnp.int32),
            pltpu.VMEM((N, HALF), jnp.bfloat16),
            pltpu.VMEM((N, HALF), jnp.bfloat16),
            pltpu.VMEM((4, LINED, LANES), jnp.float32),
            pltpu.VMEM((KX, 4, N, LANES), jnp.float32),
            pltpu.VMEM((4, KX, N, LANES), jnp.float32),
            pltpu.VMEM((4, N, LANES), jnp.float32),
            pltpu.VMEM((KX, N, LANES), jnp.float32),
            pltpu.VMEM((4, 32, MADE, LANES), jnp.float32),
            pltpu.VMEM((LANES, LANES), jnp.float32),
            pltpu.VMEM((NB, NR, 8, LANES), jnp.float32),
            pltpu.SemaphoreType.DMA((2,)),
            pltpu.SemaphoreType.DMA((4, 2)),
            pltpu.SemaphoreType.DMA,
        ],
        name="middle",
        compiler_params=pltpu.CompilerParams(vmem_limit_bytes=MIDDLE_MIB << 20),
    )(y_sizes, old_place, new_col, *matrices, received.reshape(NB, NR, SENT, LANES))


def unpack_kernel(in_ref, slab_ref, taken, slab, in_sem, slab_sem):
    def load(t):
        return pltpu.make_async_copy(
            in_ref.at[:, pl.ds(t * 8, 8), :], taken.at[t], in_sem.at[t]
        )

    def store(t):
        k, m = divmod(t, 2)
        return pltpu.make_async_copy(
            slab.at[t],
            slab_ref.at[:, pl.ds(m * 256, 256), pl.ds(k * LANES, LANES)],
            slab_sem.at[t],
        )

    for t in range(8):
        load(t).start()
    for t in range(8):
        load(t).wait()
        flat = taken.at[t].reshape(DEVICES * 8, LANES)
        for j in range(2):
            for gp in range(4):
                tile = flat[pl.ds(j * 4 + gp, DEVICES, stride=8), :].T
                slab[t, gp, j * LANES : (j + 1) * LANES, :] = tile
        store(t).start()
    for t in range(8):
        store(t).wait()


def unpack(arrived):
    anywhere = pl.BlockSpec(memory_space=pl.ANY)
    return pl.pallas_call(
        unpack_kernel,
        in_specs=[anywhere],
        out_specs=anywhere,
        out_shape=jax.ShapeDtypeStruct((4, N, N), jnp.float32),
        scratch_shapes=[
            pltpu.VMEM((8, DEVICES, 8, LANES), jnp.float32),
            pltpu.VMEM((8, 4, 256, LANES), jnp.float32),
            pltpu.SemaphoreType.DMA((8,)),
            pltpu.SemaphoreType.DMA((8,)),
        ],
        name="unpack",
        compiler_params=pltpu.CompilerParams(vmem_limit_bytes=60 << 20),
        cost_estimate=pl.CostEstimate(
            flops=N * N * N * 16, bytes_accessed=32 * N * N, transcendentals=0
        ),
    )(arrived)


def unpack_half_kernel(in_ref, out_ref):
    flat = in_ref.reshape(DEVICES * 8, LANES)
    for k in range(2):
        for yb in range(4):
            tile = flat[pl.ds(k * 4 + yb, DEVICES, stride=8), :].T
            out_ref[yb * LANES : (yb + 1) * LANES, k * LANES : (k + 1) * LANES] = tile


def unpack_half(arrived):
    return pl.pallas_call(
        unpack_half_kernel,
        grid=(1,),
        in_specs=[pl.BlockSpec((DEVICES, 8, LANES), lambda i: (0, 8, 0))],
        out_specs=pl.BlockSpec((N, HALF), lambda i: (0, 0)),
        out_shape=jax.ShapeDtypeStruct((N, HALF), jnp.float32),
        name="unpack_half",
        compiler_params=pltpu.CompilerParams(vmem_limit_bytes=60 << 20),
    )(arrived)


def join_kernel(core, mine_ref, other_ref, out_ref, sem):
    at = pl.multiple_of(core[0] * HALF, HALF)
    copies = (
        pltpu.make_async_copy(mine_ref, out_ref.at[:, pl.ds(at, HALF)], sem.at[0]),
        pltpu.make_async_copy(other_ref, out_ref.at[:, pl.ds(HALF - at, HALF)], sem.at[1]),
    )
    for copy in copies:
        copy.start()
    for copy in copies:
        copy.wait()


def join(mine, other, core):
    anywhere = pl.BlockSpec(memory_space=pl.ANY)
    return pl.pallas_call(
        join_kernel,
        in_specs=[pl.BlockSpec(memory_space=pltpu.SMEM), anywhere, anywhere],
        out_specs=anywhere,
        out_shape=jax.ShapeDtypeStruct((N, N), jnp.float32),
        scratch_shapes=[pltpu.SemaphoreType.DMA((2,))],
        name="join",
        compiler_params=pltpu.CompilerParams(vmem_limit_bytes=60 << 20),
    )(core, mine, other)


def exchange(value):
    return lax.all_to_all(value, AXES, split_axis=0, concat_axis=0, tiled=True)


def on_device(velocity, y_sizes, old_place, new_col):
    matrices = tuple(jnp.asarray(part) for part in spectral_pair())
    received = exchange(pack(velocity.reshape(3, ROWS, ZB, N), matrices))
    packed = middle(received, matrices, y_sizes, old_place, new_col)
    arrived = exchange(packed.reshape(DEVICES, PLACED, LANES))
    mine = unpack_half(arrived)
    other = lax.ppermute(mine, "col", [(c, c ^ 1) for c in range(lax.axis_size("col"))])
    slab = unpack(arrived)
    core = lax.axis_index("col") & 1
    peak = join(mine, other, jnp.full((1,), core, jnp.int32))
    return slab.reshape(2, 1, 2, N, N), peak


def solution(mesh):
    in_specs = (P(None, "col", "row", None, None, None), P(), P(), P())
    out_specs = (P("row", "col", None, None, None), P())
    return jax.shard_map(
        on_device, mesh=mesh, in_specs=in_specs, out_specs=out_specs, check_vma=False
    )
```

```python
import jax
import jax.numpy as jnp
import numpy as np
from jax import lax
from jax.experimental import pallas as pl
from jax.experimental.pallas import tpu as pltpu
from jax.sharding import PartitionSpec as P

AXES = ("col", "row")
LANES = 128
N = 512
HALF = N // 2
DEVICES = 128
KX = N // DEVICES
ROWS = 72
CAP = 36
SENT = 3 * ROWS
PLACED = 80
ZB = 32
NB = 16
NR = 8
PACK_MIB = 44
MIDDLE_MIB = 26


def spectral_pair():
    gap = (np.arange(N)[:, None] - np.arange(N)[None, :]) % N
    angle = gap * (np.pi / N)
    parity = 1.0 - 2.0 * (gap % 2)
    safe = np.where(gap == 0, 1.0, np.sin(angle))
    full = np.where(gap == 0, 0.0, parity * np.cos(angle) / safe * (2.0 / N))
    full = (full - full.T) / 2
    first, second = full[:HALF, :HALF], full[:HALF, HALF:]
    both = np.concatenate([(first + second) / 2, (first - second) / 2], axis=0)
    high = both.astype(jnp.bfloat16)
    low = (both - high.astype(np.float64)).astype(jnp.bfloat16)
    return high, low


def halves(value):
    high = value.astype(jnp.bfloat16)
    return high, (value - high.astype(jnp.float32)).astype(jnp.bfloat16)


def mul(left, right):
    return jnp.dot(left, right, preferred_element_type=jnp.float32)


def mul3(left, right):
    return mul(left[0], right[0]) + (mul(left[1], right[0]) + mul(left[0], right[1]))


def parts_of(high, low):
    return (high[:HALF], low[:HALF]), (high[HALF:], low[HALF:])


def derive_lanes(value, high, low):
    even, odd = parts_of(high, low)
    left, right = value[:, :HALF], value[:, HALF:]
    from_sum = mul3(halves(left + right), even)
    from_difference = mul3(halves(left - right), odd)
    return jnp.concatenate([-(from_sum + from_difference), from_difference - from_sum], axis=1)


def derive_rows(value, high, low):
    even, odd = parts_of(high, low)
    top, bottom = value[:HALF], value[HALF:]
    from_sum = mul3(even, halves(top + bottom))
    from_difference = mul3(odd, halves(top - bottom))
    return jnp.concatenate([from_sum + from_difference, from_sum - from_difference], axis=0)


def pack_row(value, flat, row):
    tall = jnp.concatenate([value[:, k * LANES : (k + 1) * LANES] for k in range(KX)], axis=0)
    flat[pl.ds(row, DEVICES, stride=SENT), :] = tall.T


FIELDS = (2, 1, 0)
STEPS = ROWS // 8
GROUP = 3


def pack_kernel(in_ref, high_ref, low_ref, out_ref, taken, high, low, in_sem, sem):
    flat = out_ref.reshape(DEVICES * SENT, LANES)

    def load(step):
        field, t = divmod(step, STEPS)
        return pltpu.make_async_copy(
            in_ref.at[FIELDS[field], pl.ds(t * 8, 8)], taken.at[step], in_sem.at[step]
        )

    constants = (
        pltpu.make_async_copy(high_ref, high, sem.at[0]),
        pltpu.make_async_copy(low_ref, low, sem.at[1]),
    )
    for step in range(3 * STEPS):
        load(step).start()
    for copy in constants:
        copy.start()
    for step in range(2 * STEPS):
        load(step).wait()
        for i in range(8):
            pack_row(taken[step, i], flat, step * 8 + i)
    for copy in constants:
        copy.wait()
    for group in range(2 * STEPS, 3 * STEPS, GROUP):
        for step in range(group, group + GROUP):
            load(step).wait()
        lines = taken[group : group + GROUP].reshape(GROUP * 8 * ZB, N)
        slope = derive_lanes(lines, high[...], low[...])
        for i in range(GROUP * 8):
            pack_row(slope[i * ZB : (i + 1) * ZB], flat, group * 8 + i)


def pack(velocity, matrices):
    far = pl.BlockSpec(memory_space=pltpu.HBM)
    return pl.pallas_call(
        pack_kernel,
        in_specs=[far, far, far],
        out_specs=pl.BlockSpec(memory_space=pltpu.VMEM),
        out_shape=pltpu.VMEM((DEVICES, SENT, LANES), jnp.float32),
        scratch_shapes=[
            pltpu.VMEM((3 * STEPS, 8, ZB, N), jnp.float32),
            pltpu.VMEM((N, HALF), jnp.bfloat16),
            pltpu.VMEM((N, HALF), jnp.bfloat16),
            pltpu.SemaphoreType.DMA((3 * STEPS,)),
            pltpu.SemaphoreType.DMA((2,)),
        ],
        name="pack",
        compiler_params=pltpu.CompilerParams(vmem_limit_bytes=PACK_MIB << 20),
    )(velocity, *matrices)


def turn_lanes(parts):
    lane = lax.broadcasted_iota(jnp.int32, parts[0].shape, 1)
    upper = (lane // 64) == 1
    odd = (lane // 32) % 2 == 1
    a0, a1, a2, a3 = parts
    b0 = jnp.where(upper, pltpu.roll(a2, 64, 1), a0)
    b2 = jnp.where(upper, a2, pltpu.roll(a0, 64, 1))
    b1 = jnp.where(upper, pltpu.roll(a3, 64, 1), a1)
    b3 = jnp.where(upper, a3, pltpu.roll(a1, 64, 1))
    c0 = jnp.where(odd, pltpu.roll(b1, 32, 1), b0)
    c1 = jnp.where(odd, b1, pltpu.roll(b0, 96, 1))
    c2 = jnp.where(odd, pltpu.roll(b3, 32, 1), b2)
    c3 = jnp.where(odd, b3, pltpu.roll(b2, 96, 1))
    return c0, c1, c2, c3


LINED = 560
CHUNK = 128
MADE = 72


def middle_kernel(
    sizes, places, columns, high_ref, low_ref, in_ref, out_ref,
    starts, first, high, low, lined, second, part, slope_y, total, shared, top, spread,
    sem, out_sem, peak_sem,
):
    constants = (
        pltpu.make_async_copy(high_ref, high, sem.at[0]),
        pltpu.make_async_copy(low_ref, low, sem.at[1]),
    )
    for copy in constants:
        copy.start()

    start = jnp.int32(0)
    for b in range(NB):
        starts[b] = start
        start = start + sizes[b]

    def rows_of(c, carry):
        for b in range(NB):
            place = places[c, b]
            first[c, b] = place * CAP + (place >> 1) * (SENT - ROWS)
        return carry

    lax.fori_loop(0, NB, rows_of, 0)
    flat = in_ref.reshape(NB, NR * SENT, LANES)
    made = shared.reshape(4, 32, MADE, LANES)

    def field_rows(k, quad):
        return pl.ds(pl.multiple_of((k * 4 + quad) * N, N), N)

    def line_up(item, quad, lined=lined):
        for cc in range(4):
            for b in range(NB):
                row = first[quad * 4 + cc, b] + item * ROWS
                lined[cc, pl.ds(starts[b], CAP), :] = flat[quad * 4 + cc, pl.ds(row, CAP), :]

    def store(quad, side):
        return pltpu.make_async_copy(
            made.at[quad, pl.ds(side * NB, NB), pl.ds(0, 64), :],
            out_ref.at[:, quad * 2 + side, pl.ds(0, 64), :],
            out_sem.at[quad, side],
        )

    def split_z(quad, carry):
        line_up(0, quad)
        turned = turn_lanes([lined[cc, 0:N, :] for cc in range(4)])
        for k in range(KX):
            shared[field_rows(k, quad), :] = turned[k]
        line_up(1, quad, second)
        wide = jnp.concatenate([second[cc, 0:N, :] for cc in range(4)], axis=1)
        slope = derive_rows(wide, high[...], low[...])
        for cc in range(4):
            slope_y[quad, cc] = slope[:, cc * LANES : (cc + 1) * LANES]
        return carry

    for copy in constants:
        copy.wait()
    lax.fori_loop(0, 4, split_z, 0)

    def slope_z(k, carry):
        line = jnp.concatenate([shared[field_rows(k, quad), :] for quad in range(4)], axis=1)
        slope = derive_lanes(line, high[...], low[...])
        for quad in range(4):
            part[quad, k] = slope[:, quad * LANES : (quad + 1) * LANES]
        line_up(2, k)
        turned = turn_lanes([slope_y[k, cc] + lined[cc, 0:N, :] for cc in range(4)])
        for cc in range(4):
            slope_y[k, cc] = turned[cc]
        return carry

    lax.fori_loop(0, KX, slope_z, 0)
    top[...] = jnp.zeros_like(top)
    lane = lax.broadcasted_iota(jnp.int32, (8, LANES), 1)
    lane_block = ((lane // NB) % 2) * 2 + lane // 64
    lane_column = lane % NB

    def one(quad, carry):
        order = lane_block * ZB + (lane // 32) % 2
        for cc in range(4):
            for slab in range(NB):
                hit = (lane_block == cc) & (lane_column == columns[quad * 4 + cc, slab])
                order = order + jnp.where(hit, 2 * slab, 0)
        order = jnp.concatenate([order] * (CHUNK // 8), axis=0)
        for at in range(0, N, CHUNK):
            rows = slice(at, at + CHUNK)
            for k in range(KX):
                value = slope_y[quad, k, rows, :] + part[quad, k, rows, :]
                total[k, rows, :] = jnp.take_along_axis(value, order, axis=1)
        for k in range(KX):
            for yb in range(4):
                tile = total[k, yb * LANES : (yb + 1) * LANES, :].T
                at = k * 4 + yb
                rows = made.at[quad].reshape(32 * MADE, LANES)
                for gp in range(4):
                    rows[pl.ds(at * 4 + gp, 32, stride=MADE), :] = tile[gp * 32 : (gp + 1) * 32, :]
                best = jnp.max(jnp.abs(tile).reshape(16, 8, LANES), axis=0)
                top[at * 8 : at * 8 + 8, :] = jnp.maximum(top[at * 8 : at * 8 + 8, :], best)
        for side in range(2):
            store(quad, side).start()
        return carry

    lax.fori_loop(0, 4, one, 0)
    peak = jnp.max(top[...].reshape(16, 8, LANES), axis=1)
    spread[...] = jnp.broadcast_to(peak[None, None], spread.shape)
    last = pltpu.make_async_copy(spread, out_ref.at[:, :, pl.ds(64, 16), :], peak_sem)
    last.start()
    for quad in range(4):
        for side in range(2):
            store(quad, side).wait()
    last.wait()


def middle(received, matrices, y_sizes, old_place, new_col):
    anywhere = pl.BlockSpec(memory_space=pl.ANY)
    far = pl.BlockSpec(memory_space=pltpu.HBM)
    near = pl.BlockSpec(memory_space=pltpu.SMEM)
    return pl.pallas_call(
        middle_kernel,
        in_specs=[near, near, near, far, far, pl.BlockSpec(memory_space=pltpu.VMEM)],
        out_specs=anywhere,
        out_shape=pltpu.VMEM((NB, NR, PLACED, LANES), jnp.float32),
        scratch_shapes=[
            pltpu.SMEM((NB,), jnp.int32),
            pltpu.SMEM((NB, NB), jnp.int32),
            pltpu.VMEM((N, HALF), jnp.bfloat16),
            pltpu.VMEM((N, HALF), jnp.bfloat16),
            pltpu.VMEM((4, LINED, LANES), jnp.float32),
            pltpu.VMEM((4, LINED, LANES), jnp.float32),
            pltpu.VMEM((4, KX, N, LANES), jnp.float32),
            pltpu.VMEM((4, 4, N, LANES), jnp.float32),
            pltpu.VMEM((KX, N, LANES), jnp.float32),
            pltpu.VMEM((4 * 32 * MADE, LANES), jnp.float32),
            pltpu.VMEM((LANES, LANES), jnp.float32),
            pltpu.VMEM((NB, NR, 16, LANES), jnp.float32),
            pltpu.SemaphoreType.DMA((2,)),
            pltpu.SemaphoreType.DMA((4, 2)),
            pltpu.SemaphoreType.DMA,
        ],
        name="middle",
        compiler_params=pltpu.CompilerParams(vmem_limit_bytes=MIDDLE_MIB << 20),
    )(y_sizes, old_place, new_col, *matrices, received.reshape(NB, NR, SENT, LANES))


def unpack_kernel(in_ref, slab_ref, peak_ref, taken, slab, peak, in_sem, slab_sem, peak_sem):
    def load(t):
        return pltpu.make_async_copy(
            in_ref.at[:, pl.ds(t * 8, 8), :], taken.at[t], in_sem.at[t]
        )

    def store(t):
        k, m = divmod(t, 2)
        return pltpu.make_async_copy(
            slab.at[t],
            slab_ref.at[:, pl.ds(m * 256, 256), pl.ds(k * LANES, LANES)],
            slab_sem.at[t],
        )

    def store_peak(t):
        return pltpu.make_async_copy(
            peak.at[t], peak_ref.at[:, pl.ds(t * 256, 256)], peak_sem.at[t]
        )

    def turn(t, row):
        flat = taken.at[t].reshape(DEVICES * 8, LANES)
        return flat[pl.ds(row, DEVICES, stride=8), :].T

    for t in range(10):
        load(t).start()
    for t in range(8):
        load(t).wait()
        for j in range(2):
            for gp in range(4):
                slab[t, gp, j * LANES : (j + 1) * LANES, :] = turn(t, j * 4 + gp)
        store(t).start()
    for t in range(2):
        load(8 + t).wait()
        for half in range(2):
            for yb in range(4):
                peak[t, yb * LANES : (yb + 1) * LANES, half * LANES : (half + 1) * LANES] = turn(
                    8 + t, half * 4 + yb
                )
        store_peak(t).start()
    for t in range(8):
        store(t).wait()
    for t in range(2):
        store_peak(t).wait()


def unpack(arrived):
    anywhere = pl.BlockSpec(memory_space=pl.ANY)
    return pl.pallas_call(
        unpack_kernel,
        in_specs=[anywhere],
        out_specs=[anywhere, anywhere],
        out_shape=[
            jax.ShapeDtypeStruct((4, N, N), jnp.float32),
            jax.ShapeDtypeStruct((N, N), jnp.float32),
        ],
        scratch_shapes=[
            pltpu.VMEM((10, DEVICES, 8, LANES), jnp.float32),
            pltpu.VMEM((8, 4, 256, LANES), jnp.float32),
            pltpu.VMEM((2, N, 256), jnp.float32),
            pltpu.SemaphoreType.DMA((10,)),
            pltpu.SemaphoreType.DMA((8,)),
            pltpu.SemaphoreType.DMA((2,)),
        ],
        name="unpack",
        compiler_params=pltpu.CompilerParams(vmem_limit_bytes=16 << 20),
    )(arrived)


def exchange(value):
    return lax.all_to_all(value, AXES, split_axis=0, concat_axis=0, tiled=True)


def on_device(velocity, y_sizes, old_place, new_col):
    matrices = tuple(jnp.asarray(part) for part in spectral_pair())
    received = exchange(pack(velocity.reshape(3, ROWS, ZB, N), matrices))
    packed = middle(received, matrices, y_sizes, old_place, new_col)
    slab, peak = unpack(exchange(packed.reshape(DEVICES, PLACED, LANES)))
    return slab.reshape(2, 1, 2, N, N), peak


def solution(mesh):
    in_specs = (P(None, "col", "row", None, None, None), P(), P(), P())
    out_specs = (P("row", "col", None, None, None), P())
    return jax.shard_map(
        on_device, mesh=mesh, in_specs=in_specs, out_specs=out_specs, check_vma=False
    )
```

```python
import jax
import jax.numpy as jnp
import numpy as np
from jax import lax
from jax.experimental import pallas as pl
from jax.experimental.pallas import tpu as pltpu
from jax.sharding import PartitionSpec as P

AXES = ("col", "row")
LANES = 128
N = 512
HALF = N // 2
DEVICES = 128
KX = N // DEVICES
ROWS = 72
CAP = 36
SENT = 3 * ROWS
PLACED = 80
ZB = 32
NB = 16
NR = 8
PACK_MIB = 44
MIDDLE_MIB = 26


def spectral_pair():
    gap = (np.arange(N)[:, None] - np.arange(N)[None, :]) % N
    angle = gap * (np.pi / N)
    parity = 1.0 - 2.0 * (gap % 2)
    safe = np.where(gap == 0, 1.0, np.sin(angle))
    full = np.where(gap == 0, 0.0, parity * np.cos(angle) / safe * (2.0 / N))
    full = (full - full.T) / 2
    first, second = full[:HALF, :HALF], full[:HALF, HALF:]
    both = np.concatenate([(first + second) / 2, (first - second) / 2], axis=0)
    high = both.astype(jnp.bfloat16)
    low = (both - high.astype(np.float64)).astype(jnp.bfloat16)
    return high, low


def halves(value):
    high = value.astype(jnp.bfloat16)
    return high, (value - high.astype(jnp.float32)).astype(jnp.bfloat16)


def mul(left, right):
    return jnp.dot(left, right, preferred_element_type=jnp.float32)


def mul3(left, right):
    return mul(left[0], right[0]) + (mul(left[1], right[0]) + mul(left[0], right[1]))


def parts_of(high, low):
    return (high[:HALF], low[:HALF]), (high[HALF:], low[HALF:])


def derive_lanes(value, high, low):
    even, odd = parts_of(high, low)
    left, right = value[:, :HALF], value[:, HALF:]
    from_sum = mul3(halves(left + right), even)
    from_difference = mul3(halves(left - right), odd)
    return jnp.concatenate([-(from_sum + from_difference), from_difference - from_sum], axis=1)


def derive_rows(value, high, low):
    even, odd = parts_of(high, low)
    top, bottom = value[:HALF], value[HALF:]
    from_sum = mul3(even, halves(top + bottom))
    from_difference = mul3(odd, halves(top - bottom))
    return jnp.concatenate([from_sum + from_difference, from_sum - from_difference], axis=0)


def pack_row(value, flat, row):
    tall = jnp.concatenate([value[:, k * LANES : (k + 1) * LANES] for k in range(KX)], axis=0)
    flat[pl.ds(row, DEVICES, stride=SENT), :] = tall.T


FIELDS = (2, 1, 0)
STEPS = ROWS // 8
GROUP = 3


def pack_kernel(in_ref, high_ref, low_ref, out_ref, taken, high, low, in_sem, sem):
    flat = out_ref.reshape(DEVICES * SENT, LANES)

    def load(step):
        field, t = divmod(step, STEPS)
        return pltpu.make_async_copy(
            in_ref.at[FIELDS[field], pl.ds(t * 8, 8)], taken.at[step], in_sem.at[step]
        )

    constants = (
        pltpu.make_async_copy(high_ref, high, sem.at[0]),
        pltpu.make_async_copy(low_ref, low, sem.at[1]),
    )
    groups = [range(group, group + GROUP) for group in range(0, STEPS, GROUP)]
    for step in range(STEPS):
        load(step).start()
    for copy in constants:
        copy.start()
    for group in groups:
        for item in (2, 1):
            for step in group:
                load(item * STEPS + step).start()

    for step in range(STEPS):
        load(step).wait()
        for i in range(8):
            pack_row(taken[step, i], flat, step * 8 + i)
    for copy in constants:
        copy.wait()
    for group in groups:
        for item in (2, 1):
            for step in group:
                load(item * STEPS + step).wait()
        at = 2 * STEPS + group[0]
        lines = taken[at : at + GROUP].reshape(GROUP * 8 * ZB, N)
        slope = derive_lanes(lines, high[...], low[...])
        for step in group:
            for i in range(8):
                pack_row(taken[STEPS + step, i], flat, (STEPS + step) * 8 + i)
        for i in range(GROUP * 8):
            pack_row(slope[i * ZB : (i + 1) * ZB], flat, at * 8 + i)


def pack(velocity, matrices):
    far = pl.BlockSpec(memory_space=pltpu.HBM)
    return pl.pallas_call(
        pack_kernel,
        in_specs=[far, far, far],
        out_specs=pl.BlockSpec(memory_space=pltpu.VMEM),
        out_shape=pltpu.VMEM((DEVICES, SENT, LANES), jnp.float32),
        scratch_shapes=[
            pltpu.VMEM((3 * STEPS, 8, ZB, N), jnp.float32),
            pltpu.VMEM((N, HALF), jnp.bfloat16),
            pltpu.VMEM((N, HALF), jnp.bfloat16),
            pltpu.SemaphoreType.DMA((3 * STEPS,)),
            pltpu.SemaphoreType.DMA((2,)),
        ],
        name="pack",
        compiler_params=pltpu.CompilerParams(vmem_limit_bytes=PACK_MIB << 20),
    )(velocity, *matrices)


def turn_lanes(parts):
    lane = lax.broadcasted_iota(jnp.int32, parts[0].shape, 1)
    upper = (lane // 64) == 1
    odd = (lane // 32) % 2 == 1
    a0, a1, a2, a3 = parts
    b0 = jnp.where(upper, pltpu.roll(a2, 64, 1), a0)
    b2 = jnp.where(upper, a2, pltpu.roll(a0, 64, 1))
    b1 = jnp.where(upper, pltpu.roll(a3, 64, 1), a1)
    b3 = jnp.where(upper, a3, pltpu.roll(a1, 64, 1))
    c0 = jnp.where(odd, pltpu.roll(b1, 32, 1), b0)
    c1 = jnp.where(odd, b1, pltpu.roll(b0, 96, 1))
    c2 = jnp.where(odd, pltpu.roll(b3, 32, 1), b2)
    c3 = jnp.where(odd, b3, pltpu.roll(b2, 96, 1))
    return c0, c1, c2, c3


LINED = 560
CHUNK = 128
MADE = 72


def middle_kernel(
    sizes, places, columns, high_ref, low_ref, in_ref, out_ref,
    starts, first, high, low, lined, second, part, slope_y, total, shared, top, spread,
    sem, out_sem, peak_sem,
):
    constants = (
        pltpu.make_async_copy(high_ref, high, sem.at[0]),
        pltpu.make_async_copy(low_ref, low, sem.at[1]),
    )
    for copy in constants:
        copy.start()

    start = jnp.int32(0)
    for b in range(NB):
        starts[b] = start
        start = start + sizes[b]

    def rows_of(c, carry):
        for b in range(NB):
            place = places[c, b]
            first[c, b] = place * CAP + (place >> 1) * (SENT - ROWS)
        return carry

    lax.fori_loop(0, NB, rows_of, 0)
    flat = in_ref.reshape(NB, NR * SENT, LANES)
    made = shared.reshape(4, 32, MADE, LANES)

    def field_rows(k, quad):
        return pl.ds(pl.multiple_of((k * 4 + quad) * N, N), N)

    def line_up(item, quad, lined=lined):
        for cc in range(4):
            for b in range(NB):
                row = first[quad * 4 + cc, b] + item * ROWS
                lined[cc, pl.ds(starts[b], CAP), :] = flat[quad * 4 + cc, pl.ds(row, CAP), :]

    def store(quad, side):
        return pltpu.make_async_copy(
            made.at[quad, pl.ds(side * NB, NB), pl.ds(0, 64), :],
            out_ref.at[:, quad * 2 + side, pl.ds(0, 64), :],
            out_sem.at[quad, side],
        )

    def split_z(quad, carry):
        line_up(0, quad)
        turned = turn_lanes([lined[cc, 0:N, :] for cc in range(4)])
        for k in range(KX):
            shared[field_rows(k, quad), :] = turned[k]
        line_up(1, quad, second)
        wide = jnp.concatenate([second[cc, 0:N, :] for cc in range(4)], axis=1)
        slope = derive_rows(wide, high[...], low[...])
        for cc in range(4):
            slope_y[quad, cc] = slope[:, cc * LANES : (cc + 1) * LANES]
        return carry

    for copy in constants:
        copy.wait()
    lax.fori_loop(0, 4, split_z, 0)

    def slope_z(k, carry):
        line = jnp.concatenate([shared[field_rows(k, quad), :] for quad in range(4)], axis=1)
        slope = derive_lanes(line, high[...], low[...])
        for quad in range(4):
            part[quad, k] = slope[:, quad * LANES : (quad + 1) * LANES]
        line_up(2, k)
        turned = turn_lanes([slope_y[k, cc] + lined[cc, 0:N, :] for cc in range(4)])
        for cc in range(4):
            slope_y[k, cc] = turned[cc]
        return carry

    lax.fori_loop(0, KX, slope_z, 0)
    top[...] = jnp.zeros_like(top)
    lane = lax.broadcasted_iota(jnp.int32, (8, LANES), 1)
    lane_block = ((lane // NB) % 2) * 2 + lane // 64
    lane_column = lane % NB

    def one(quad, carry):
        order = lane_block * ZB + (lane // 32) % 2
        for cc in range(4):
            for slab in range(NB):
                hit = (lane_block == cc) & (lane_column == columns[quad * 4 + cc, slab])
                order = order + jnp.where(hit, 2 * slab, 0)
        order = jnp.concatenate([order] * (CHUNK // 8), axis=0)
        for at in range(0, N, CHUNK):
            rows = slice(at, at + CHUNK)
            for k in range(KX):
                value = slope_y[quad, k, rows, :] + part[quad, k, rows, :]
                total[k, rows, :] = jnp.take_along_axis(value, order, axis=1)
        for k in range(KX):
            for yb in range(4):
                tile = total[k, yb * LANES : (yb + 1) * LANES, :].T
                at = k * 4 + yb
                rows = made.at[quad].reshape(32 * MADE, LANES)
                for gp in range(4):
                    rows[pl.ds(at * 4 + gp, 32, stride=MADE), :] = tile[gp * 32 : (gp + 1) * 32, :]
                best = jnp.max(jnp.abs(tile).reshape(16, 8, LANES), axis=0)
                top[at * 8 : at * 8 + 8, :] = jnp.maximum(top[at * 8 : at * 8 + 8, :], best)
        for side in range(2):
            store(quad, side).start()
        return carry

    lax.fori_loop(0, 4, one, 0)
    peak = jnp.max(top[...].reshape(16, 8, LANES), axis=1)
    spread[...] = jnp.broadcast_to(peak[None, None], spread.shape)
    last = pltpu.make_async_copy(spread, out_ref.at[:, :, pl.ds(64, 16), :], peak_sem)
    last.start()
    for quad in range(4):
        for side in range(2):
            store(quad, side).wait()
    last.wait()


def middle(received, matrices, y_sizes, old_place, new_col):
    anywhere = pl.BlockSpec(memory_space=pl.ANY)
    far = pl.BlockSpec(memory_space=pltpu.HBM)
    near = pl.BlockSpec(memory_space=pltpu.SMEM)
    return pl.pallas_call(
        middle_kernel,
        in_specs=[near, near, near, far, far, pl.BlockSpec(memory_space=pltpu.VMEM)],
        out_specs=anywhere,
        out_shape=pltpu.VMEM((NB, NR, PLACED, LANES), jnp.float32),
        scratch_shapes=[
            pltpu.SMEM((NB,), jnp.int32),
            pltpu.SMEM((NB, NB), jnp.int32),
            pltpu.VMEM((N, HALF), jnp.bfloat16),
            pltpu.VMEM((N, HALF), jnp.bfloat16),
            pltpu.VMEM((4, LINED, LANES), jnp.float32),
            pltpu.VMEM((4, LINED, LANES), jnp.float32),
            pltpu.VMEM((4, KX, N, LANES), jnp.float32),
            pltpu.VMEM((4, 4, N, LANES), jnp.float32),
            pltpu.VMEM((KX, N, LANES), jnp.float32),
            pltpu.VMEM((4 * 32 * MADE, LANES), jnp.float32),
            pltpu.VMEM((LANES, LANES), jnp.float32),
            pltpu.VMEM((NB, NR, 16, LANES), jnp.float32),
            pltpu.SemaphoreType.DMA((2,)),
            pltpu.SemaphoreType.DMA((4, 2)),
            pltpu.SemaphoreType.DMA,
        ],
        name="middle",
        compiler_params=pltpu.CompilerParams(vmem_limit_bytes=MIDDLE_MIB << 20),
    )(y_sizes, old_place, new_col, *matrices, received.reshape(NB, NR, SENT, LANES))


def unpack_kernel(in_ref, slab_ref, peak_ref, taken, slab, peak, in_sem, slab_sem, peak_sem):
    def load(t):
        return pltpu.make_async_copy(
            in_ref.at[:, pl.ds(t * 8, 8), :], taken.at[t], in_sem.at[t]
        )

    def store(yb):
        return pltpu.make_async_copy(
            slab.at[yb], slab_ref.at[:, pl.ds(yb * LANES, LANES), :], slab_sem.at[yb]
        )

    def turn(t, row):
        flat = taken.at[t].reshape(DEVICES * 8, LANES)
        return flat[pl.ds(row, DEVICES, stride=8), :].T

    for m in range(2):
        for k in range(KX):
            load(k * 2 + m).start()
    for t in range(2):
        load(8 + t).start()
    for m in range(2):
        for k in range(KX):
            load(k * 2 + m).wait()
        for j in range(2):
            yb = m * 2 + j
            for gp in range(4):
                for k in range(KX):
                    slab[yb, gp, :, k * LANES : (k + 1) * LANES] = turn(k * 2 + m, j * 4 + gp)
            store(yb).start()
    for t in range(2):
        load(8 + t).wait()
        for half in range(2):
            for yb in range(4):
                k = t * 2 + half
                rows = slice(yb * LANES, (yb + 1) * LANES)
                peak[rows, k * LANES : (k + 1) * LANES] = turn(8 + t, half * 4 + yb)
    last = pltpu.make_async_copy(peak, peak_ref, peak_sem)
    last.start()
    for yb in range(4):
        store(yb).wait()
    last.wait()


def unpack(arrived):
    anywhere = pl.BlockSpec(memory_space=pl.ANY)
    return pl.pallas_call(
        unpack_kernel,
        in_specs=[anywhere],
        out_specs=[anywhere, anywhere],
        out_shape=[
            jax.ShapeDtypeStruct((4, N, N), jnp.float32),
            jax.ShapeDtypeStruct((N, N), jnp.float32),
        ],
        scratch_shapes=[
            pltpu.VMEM((10, DEVICES, 8, LANES), jnp.float32),
            pltpu.VMEM((4, 4, LANES, N), jnp.float32),
            pltpu.VMEM((N, N), jnp.float32),
            pltpu.SemaphoreType.DMA((10,)),
            pltpu.SemaphoreType.DMA((4,)),
            pltpu.SemaphoreType.DMA,
        ],
        name="unpack",
        compiler_params=pltpu.CompilerParams(vmem_limit_bytes=16 << 20),
    )(arrived)


def exchange(value):
    return lax.all_to_all(value, AXES, split_axis=0, concat_axis=0, tiled=True)


def on_device(velocity, y_sizes, old_place, new_col):
    matrices = tuple(jnp.asarray(part) for part in spectral_pair())
    received = exchange(pack(velocity.reshape(3, ROWS, ZB, N), matrices))
    packed = middle(received, matrices, y_sizes, old_place, new_col)
    slab, peak = unpack(exchange(packed.reshape(DEVICES, PLACED, LANES)))
    return slab.reshape(2, 1, 2, N, N), peak


def solution(mesh):
    in_specs = (P(None, "col", "row", None, None, None), P(), P(), P())
    out_specs = (P("row", "col", None, None, None), P())
    return jax.shard_map(
        on_device, mesh=mesh, in_specs=in_specs, out_specs=out_specs, check_vma=False
    )
```

```python
import jax
import jax.numpy as jnp
import numpy as np
from jax import lax
from jax.experimental import pallas as pl
from jax.experimental.pallas import tpu as pltpu
from jax.sharding import PartitionSpec as P

AXES = ("col", "row")
LANES = 128
N = 512
HALF = N // 2
DEVICES = 128
KX = N // DEVICES
ROWS = 72
CAP = 36
SENT = 3 * ROWS
PLACED = 80
ZB = 32
NB = 16
NR = 8
PACK_MIB = 44
MIDDLE_MIB = 26


def spectral_pair():
    gap = (np.arange(N)[:, None] - np.arange(N)[None, :]) % N
    angle = gap * (np.pi / N)
    parity = 1.0 - 2.0 * (gap % 2)
    safe = np.where(gap == 0, 1.0, np.sin(angle))
    full = np.where(gap == 0, 0.0, parity * np.cos(angle) / safe * (2.0 / N))
    full = (full - full.T) / 2
    first, second = full[:HALF, :HALF], full[:HALF, HALF:]
    both = np.concatenate([(first + second) / 2, (first - second) / 2], axis=0)
    high = both.astype(jnp.bfloat16)
    low = (both - high.astype(np.float64)).astype(jnp.bfloat16)
    return high, low


def halves(value):
    high = value.astype(jnp.bfloat16)
    return high, (value - high.astype(jnp.float32)).astype(jnp.bfloat16)


def mul(left, right):
    return jnp.dot(left, right, preferred_element_type=jnp.float32)


def mul3(left, right):
    return mul(left[0], right[0]) + (mul(left[1], right[0]) + mul(left[0], right[1]))


def parts_of(high, low):
    return (high[:HALF], low[:HALF]), (high[HALF:], low[HALF:])


def derive_lanes(value, high, low):
    even, odd = parts_of(high, low)
    left, right = value[:, :HALF], value[:, HALF:]
    from_sum = mul3(halves(left + right), even)
    from_difference = mul3(halves(left - right), odd)
    return jnp.concatenate([-(from_sum + from_difference), from_difference - from_sum], axis=1)


def derive_rows(value, high, low):
    even, odd = parts_of(high, low)
    top, bottom = value[:HALF], value[HALF:]
    from_sum = mul3(even, halves(top + bottom))
    from_difference = mul3(odd, halves(top - bottom))
    return jnp.concatenate([from_sum + from_difference, from_sum - from_difference], axis=0)


def pack_row(value, flat, row):
    tall = jnp.concatenate([value[:, k * LANES : (k + 1) * LANES] for k in range(KX)], axis=0)
    flat[pl.ds(row, DEVICES, stride=SENT), :] = tall.T


FIELDS = (2, 1, 0)
STEPS = ROWS // 8
GROUP = 3


def pack_kernel(in_ref, high_ref, low_ref, out_ref, taken, high, low, in_sem, sem):
    flat = out_ref.reshape(DEVICES * SENT, LANES)

    def load(step):
        field, t = divmod(step, STEPS)
        return pltpu.make_async_copy(
            in_ref.at[FIELDS[field], pl.ds(t * 8, 8)], taken.at[step], in_sem.at[step]
        )

    constants = (
        pltpu.make_async_copy(high_ref, high, sem.at[0]),
        pltpu.make_async_copy(low_ref, low, sem.at[1]),
    )
    groups = [range(group, group + GROUP) for group in range(0, STEPS, GROUP)]
    for step in range(STEPS):
        load(step).start()
    for copy in constants:
        copy.start()
    for group in groups:
        for item in (2, 1):
            for step in group:
                load(item * STEPS + step).start()

    for step in range(STEPS):
        load(step).wait()
        for i in range(8):
            pack_row(taken[step, i], flat, step * 8 + i)
    for copy in constants:
        copy.wait()
    for group in groups:
        for item in (2, 1):
            for step in group:
                load(item * STEPS + step).wait()
        at = 2 * STEPS + group[0]
        lines = taken[at : at + GROUP].reshape(GROUP * 8 * ZB, N)
        slope = derive_lanes(lines, high[...], low[...])
        for step in group:
            for i in range(8):
                pack_row(taken[STEPS + step, i], flat, (STEPS + step) * 8 + i)
        for i in range(GROUP * 8):
            pack_row(slope[i * ZB : (i + 1) * ZB], flat, at * 8 + i)


def pack(velocity, matrices):
    far = pl.BlockSpec(memory_space=pltpu.HBM)
    return pl.pallas_call(
        pack_kernel,
        in_specs=[far, far, far],
        out_specs=pl.BlockSpec(memory_space=pltpu.VMEM),
        out_shape=pltpu.VMEM((DEVICES, SENT, LANES), jnp.float32),
        scratch_shapes=[
            pltpu.VMEM((3 * STEPS, 8, ZB, N), jnp.float32),
            pltpu.VMEM((N, HALF), jnp.bfloat16),
            pltpu.VMEM((N, HALF), jnp.bfloat16),
            pltpu.SemaphoreType.DMA((3 * STEPS,)),
            pltpu.SemaphoreType.DMA((2,)),
        ],
        name="pack",
        compiler_params=pltpu.CompilerParams(vmem_limit_bytes=PACK_MIB << 20),
    )(velocity, *matrices)


def turn_lanes(parts):
    lane = lax.broadcasted_iota(jnp.int32, parts[0].shape, 1)
    upper = (lane // 64) == 1
    odd = (lane // 32) % 2 == 1
    a0, a1, a2, a3 = parts
    b0 = jnp.where(upper, pltpu.roll(a2, 64, 1), a0)
    b2 = jnp.where(upper, a2, pltpu.roll(a0, 64, 1))
    b1 = jnp.where(upper, pltpu.roll(a3, 64, 1), a1)
    b3 = jnp.where(upper, a3, pltpu.roll(a1, 64, 1))
    c0 = jnp.where(odd, pltpu.roll(b1, 32, 1), b0)
    c1 = jnp.where(odd, b1, pltpu.roll(b0, 96, 1))
    c2 = jnp.where(odd, pltpu.roll(b3, 32, 1), b2)
    c3 = jnp.where(odd, b3, pltpu.roll(b2, 96, 1))
    return c0, c1, c2, c3


LINED = 560
CHUNK = 128
MADE = 72


def middle_kernel(
    sizes, places, columns, high_ref, low_ref, in_ref, out_ref,
    starts, first, high, low, lined, second, part, slope_y, total, shared, top, spread,
    sem, out_sem, peak_sem,
):
    constants = (
        pltpu.make_async_copy(high_ref, high, sem.at[0]),
        pltpu.make_async_copy(low_ref, low, sem.at[1]),
    )
    for copy in constants:
        copy.start()

    start = jnp.int32(0)
    for b in range(NB):
        starts[b] = start
        start = start + sizes[b]

    def rows_of(c, carry):
        for b in range(NB):
            place = places[c, b]
            first[c, b] = place * CAP + (place >> 1) * (SENT - ROWS)
        return carry

    lax.fori_loop(0, NB, rows_of, 0)
    flat = in_ref.reshape(NB, NR * SENT, LANES)
    made = shared.reshape(4, 32, MADE, LANES)

    def field_rows(k, quad):
        return pl.ds(pl.multiple_of((k * 4 + quad) * N, N), N)

    def line_up(item, quad, lined=lined):
        for cc in range(4):
            for b in range(NB):
                row = first[quad * 4 + cc, b] + item * ROWS
                lined[cc, pl.ds(starts[b], CAP), :] = flat[quad * 4 + cc, pl.ds(row, CAP), :]

    def store(quad, side):
        return pltpu.make_async_copy(
            made.at[quad, pl.ds(side * NB, NB), pl.ds(0, 64), :],
            out_ref.at[:, quad * 2 + side, pl.ds(0, 64), :],
            out_sem.at[quad, side],
        )

    def split_z(quad, carry):
        line_up(0, quad)
        turned = turn_lanes([lined[cc, 0:N, :] for cc in range(4)])
        for k in range(KX):
            shared[field_rows(k, quad), :] = turned[k]
        line_up(1, quad, second)
        wide = jnp.concatenate([second[cc, 0:N, :] for cc in range(4)], axis=1)
        slope = derive_rows(wide, high[...], low[...])
        for cc in range(4):
            slope_y[quad, cc] = slope[:, cc * LANES : (cc + 1) * LANES]
        return carry

    for copy in constants:
        copy.wait()
    lax.fori_loop(0, 4, split_z, 0)

    def slope_z(k, carry):
        line = jnp.concatenate([shared[field_rows(k, quad), :] for quad in range(4)], axis=1)
        slope = derive_lanes(line, high[...], low[...])
        for quad in range(4):
            part[quad, k] = slope[:, quad * LANES : (quad + 1) * LANES]
        line_up(2, k)
        turned = turn_lanes([slope_y[k, cc] + lined[cc, 0:N, :] for cc in range(4)])
        for cc in range(4):
            slope_y[k, cc] = turned[cc]
        return carry

    lax.fori_loop(0, KX, slope_z, 0)
    top[...] = jnp.zeros_like(top)
    lane = lax.broadcasted_iota(jnp.int32, (8, LANES), 1)
    lane_block = ((lane // NB) % 2) * 2 + lane // 64
    lane_column = lane % NB

    def one(quad, carry):
        order = lane_block * ZB + (lane // 32) % 2
        for cc in range(4):
            for slab in range(NB):
                hit = (lane_block == cc) & (lane_column == columns[quad * 4 + cc, slab])
                order = order + jnp.where(hit, 2 * slab, 0)
        order = jnp.concatenate([order] * (CHUNK // 8), axis=0)
        for at in range(0, N, CHUNK):
            rows = slice(at, at + CHUNK)
            for k in range(KX):
                value = slope_y[quad, k, rows, :] + part[quad, k, rows, :]
                total[k, rows, :] = jnp.take_along_axis(value, order, axis=1)
        for k in range(KX):
            for yb in range(4):
                tile = total[k, yb * LANES : (yb + 1) * LANES, :].T
                at = k * 4 + yb
                rows = made.at[quad].reshape(32 * MADE, LANES)
                for gp in range(4):
                    rows[pl.ds(at * 4 + gp, 32, stride=MADE), :] = tile[gp * 32 : (gp + 1) * 32, :]
                best = jnp.max(jnp.abs(tile).reshape(16, 8, LANES), axis=0)
                top[at * 8 : at * 8 + 8, :] = jnp.maximum(top[at * 8 : at * 8 + 8, :], best)
        for side in range(2):
            store(quad, side).start()
        return carry

    lax.fori_loop(0, 4, one, 0, unroll=2)
    peak = jnp.max(top[...].reshape(16, 8, LANES), axis=1)
    spread[...] = jnp.broadcast_to(peak[None, None], spread.shape)
    last = pltpu.make_async_copy(spread, out_ref.at[:, :, pl.ds(64, 16), :], peak_sem)
    last.start()
    for quad in range(4):
        for side in range(2):
            store(quad, side).wait()
    last.wait()


def middle(received, matrices, y_sizes, old_place, new_col):
    anywhere = pl.BlockSpec(memory_space=pl.ANY)
    far = pl.BlockSpec(memory_space=pltpu.HBM)
    near = pl.BlockSpec(memory_space=pltpu.SMEM)
    return pl.pallas_call(
        middle_kernel,
        in_specs=[near, near, near, far, far, pl.BlockSpec(memory_space=pltpu.VMEM)],
        out_specs=anywhere,
        out_shape=pltpu.VMEM((NB, NR, PLACED, LANES), jnp.float32),
        scratch_shapes=[
            pltpu.SMEM((NB,), jnp.int32),
            pltpu.SMEM((NB, NB), jnp.int32),
            pltpu.VMEM((N, HALF), jnp.bfloat16),
            pltpu.VMEM((N, HALF), jnp.bfloat16),
            pltpu.VMEM((4, LINED, LANES), jnp.float32),
            pltpu.VMEM((4, LINED, LANES), jnp.float32),
            pltpu.VMEM((4, KX, N, LANES), jnp.float32),
            pltpu.VMEM((4, 4, N, LANES), jnp.float32),
            pltpu.VMEM((KX, N, LANES), jnp.float32),
            pltpu.VMEM((4 * 32 * MADE, LANES), jnp.float32),
            pltpu.VMEM((LANES, LANES), jnp.float32),
            pltpu.VMEM((NB, NR, 16, LANES), jnp.float32),
            pltpu.SemaphoreType.DMA((2,)),
            pltpu.SemaphoreType.DMA((4, 2)),
            pltpu.SemaphoreType.DMA,
        ],
        name="middle",
        compiler_params=pltpu.CompilerParams(vmem_limit_bytes=MIDDLE_MIB << 20),
    )(y_sizes, old_place, new_col, *matrices, received.reshape(NB, NR, SENT, LANES))


def unpack_kernel(in_ref, slab_ref, peak_ref, taken, slab, peak, in_sem, slab_sem, peak_sem):
    def load(t):
        return pltpu.make_async_copy(
            in_ref.at[:, pl.ds(t * 8, 8), :], taken.at[t], in_sem.at[t]
        )

    def store(yb):
        return pltpu.make_async_copy(
            slab.at[yb], slab_ref.at[:, pl.ds(yb * LANES, LANES), :], slab_sem.at[yb]
        )

    def turn(t, row):
        flat = taken.at[t].reshape(DEVICES * 8, LANES)
        return flat[pl.ds(row, DEVICES, stride=8), :].T

    for m in range(2):
        for k in range(KX):
            load(k * 2 + m).start()
    for t in range(2):
        load(8 + t).start()
    for m in range(2):
        for k in range(KX):
            load(k * 2 + m).wait()
        for j in range(2):
            yb = m * 2 + j
            for gp in range(4):
                for k in range(KX):
                    slab[yb, gp, :, k * LANES : (k + 1) * LANES] = turn(k * 2 + m, j * 4 + gp)
            store(yb).start()
    for t in range(2):
        load(8 + t).wait()
        for half in range(2):
            for yb in range(4):
                k = t * 2 + half
                rows = slice(yb * LANES, (yb + 1) * LANES)
                peak[rows, k * LANES : (k + 1) * LANES] = turn(8 + t, half * 4 + yb)
    last = pltpu.make_async_copy(peak, peak_ref, peak_sem)
    last.start()
    for yb in range(4):
        store(yb).wait()
    last.wait()


def unpack(arrived):
    anywhere = pl.BlockSpec(memory_space=pl.ANY)
    return pl.pallas_call(
        unpack_kernel,
        in_specs=[anywhere],
        out_specs=[anywhere, anywhere],
        out_shape=[
            jax.ShapeDtypeStruct((4, N, N), jnp.float32),
            jax.ShapeDtypeStruct((N, N), jnp.float32),
        ],
        scratch_shapes=[
            pltpu.VMEM((10, DEVICES, 8, LANES), jnp.float32),
            pltpu.VMEM((4, 4, LANES, N), jnp.float32),
            pltpu.VMEM((N, N), jnp.float32),
            pltpu.SemaphoreType.DMA((10,)),
            pltpu.SemaphoreType.DMA((4,)),
            pltpu.SemaphoreType.DMA,
        ],
        name="unpack",
        compiler_params=pltpu.CompilerParams(vmem_limit_bytes=16 << 20),
    )(arrived)


def exchange(value):
    return lax.all_to_all(value, AXES, split_axis=0, concat_axis=0, tiled=True)


def on_device(velocity, y_sizes, old_place, new_col):
    matrices = tuple(jnp.asarray(part) for part in spectral_pair())
    received = exchange(pack(velocity.reshape(3, ROWS, ZB, N), matrices))
    packed = middle(received, matrices, y_sizes, old_place, new_col)
    slab, peak = unpack(exchange(packed.reshape(DEVICES, PLACED, LANES)))
    return slab.reshape(2, 1, 2, N, N), peak


def solution(mesh):
    in_specs = (P(None, "col", "row", None, None, None), P(), P(), P())
    out_specs = (P("row", "col", None, None, None), P())
    return jax.shard_map(
        on_device, mesh=mesh, in_specs=in_specs, out_specs=out_specs, check_vma=False
    )
```
